128 devices in a mesh: dom: 128 (over z, y, x, core).
Axes of the slice: x: 4, y: 4, z: 4, core: 2. Of those that a mesh axis runs over, the one named last changes fastest.
Arguments:
- features: bfloat16 [131072, 256], P('dom'), may hold values from -6 to 6
- edge_source: int32 [128, 128, 128], P('dom'), may hold values from 0 to 5119, as said below
- edge_relation: int32 [128, 128, 128], P('dom'), may hold values from 0 to 7
- edge_target: int32 [128, 128, 128], P('dom'), may hold values from 0 to 1023, as said below
- block_count: int32 [128], P('dom'), may hold values from 1 to 128, as said below
- send_list: int32 [128, 128, 32], P('dom'), may hold values from 0 to 1023
- bases_first: bfloat16 [30, 256, 256], P(None, 'dom'), may hold values from -0.375 to 0.375
- self_first: bfloat16 [256, 256], P('dom'), may hold values from -0.375 to 0.375
- coef_first: float32 [8, 30], replicated, may hold values from -1 to 1
- bias_first: float32 [256], replicated, may hold values from -3 to 3
- bases_second: bfloat16 [30, 256, 256], P(None, 'dom'), may hold values from -0.375 to 0.375
- self_second: bfloat16 [256, 256], P('dom'), may hold values from -0.375 to 0.375
- coef_second: float32 [8, 30], replicated, may hold values from -1 to 1
- bias_second: float32 [256], replicated, may hold values from -3 to 3
Outputs:
- embedded: bfloat16 [131072, 256], P('dom')
The draws below stay inside these ranges and needn't reach their ends.
Inputs may be any that keep to these rules, and one draw needn't show every extreme that they name: `edge_source`: an entry below 1024 names a row of the edge's own partition; an entry 1024 + p * 32 + s names the row that partition p sends to the edge's partition in slot s, and p is never the edge's own partition. `edge_target`: non-decreasing within each block; all targets of one block lie in one aligned window of 16 rows, from 16 * k to 16 * k + 15 for some k. `block_count`: blocks at and beyond it are ignored; some partition uses all 128.
All inputs are finite; a program needn't handle non-finite values.
Results may differ from the reference program's by a relative error of at most 0.0064.
Values may be sent and summed in bfloat16 or wider, within the bound.
A program may use at most 128 MiB of HBM per device.

```python
import jax
import jax.numpy as jnp
from jax import lax

D = 256
REL = 8
BASES = 30
NODE_DEV = 1024
SLOT = 32
BLOCKS = 128
EBLK = 128
WIN = 16
NODES = 131072
N_DOM = 128


def draw_edge_source(key, part):
    key_used, key_local, key_offset, key_slot, key_remote = jax.random.split(key, 5)
    shape = (N_DOM, BLOCKS, EBLK)
    sent_counts = jax.random.randint(key_used, (N_DOM, N_DOM), SLOT // 4, SLOT + 1)
    local_rows = jax.random.randint(key_local, shape, 0, NODE_DEV)
    offset = jax.random.randint(key_offset, shape, 1, N_DOM)
    target_part = jnp.arange(N_DOM, dtype=jnp.int32)[:, None, None]
    owner = (target_part + offset) % N_DOM
    limit = sent_counts[owner, target_part]
    slot_index = jax.random.randint(key_slot, shape, 0, 1 << 20) % limit
    remote = jax.random.randint(key_remote, shape, 0, 2) == 1
    return jnp.where(remote, NODE_DEV + owner * SLOT + slot_index, local_rows).astype(jnp.int32)


def draw_edge_target(key, part):
    key_window, key_offset = jax.random.split(key)
    windows = jnp.sort(jax.random.randint(key_window, (N_DOM, BLOCKS), 0, NODE_DEV // WIN), axis=1)
    offsets = jnp.sort(jax.random.randint(key_offset, (N_DOM, BLOCKS, EBLK), 0, WIN), axis=2)
    return (windows[:, :, None] * WIN + offsets).astype(jnp.int32)


def draw_block_count(key, part):
    key_counts, key_top = jax.random.split(key)
    counts = jax.random.randint(key_counts, (N_DOM,), max(BLOCKS // 2, 1), BLOCKS + 1)
    busiest = jax.random.randint(key_top, (), 0, N_DOM)
    return counts.at[busiest].set(BLOCKS).astype(jnp.int32)


def place_ends(entries, own_key, least, largest):
    spot = [jax.random.randint(jax.random.fold_in(own_key, axis), (), 0, length) for axis, length in enumerate(entries.shape)]
    main_axis = entries.shape.index(max(entries.shape))
    next_to = spot[:main_axis] + [(spot[main_axis] + 1) % entries.shape[main_axis]] + spot[main_axis + 1:]
    return entries.at[tuple(spot)].set(least).at[tuple(next_to)].set(largest)


def steps_of(own_key, shape, cuts, least, top_value):
    loudness = 1.0
    for dim, blocks in cuts:
        heights = jax.random.uniform(jax.random.fold_in(jax.random.fold_in(own_key, 6), dim), (blocks,), jnp.float32, least / len(cuts), top_value / len(cuts))
        loudness = loudness * jnp.repeat(jnp.exp(heights), shape[dim] // blocks).reshape((-1,) + (1,) * (len(shape) - 1 - dim))
    return loudness


def scatter_about(rng, dims, deviation, most, pieces=(), kind=jnp.bfloat16):
    drawn = deviation * jax.random.normal(rng, dims, jnp.float32)
    if pieces:
        drawn = drawn * steps_of(rng, dims, pieces, -0.22, 0.18)
    return jnp.clip(drawn, -most, most).astype(kind)


def setup_inputs(seed: int = 0) -> dict:
    streams_of = jax.random.split(jax.random.key(seed), 15)
    return {
        "features": scatter_about(streams_of[0], (NODES, D), 1.0, 6.0, ((0, 128),)),
        "edge_source": draw_edge_source(jax.random.fold_in(streams_of[14], 71), 0),
        "edge_relation": place_ends(jax.random.randint(streams_of[2], (N_DOM, BLOCKS, EBLK), 0, REL), jax.random.fold_in(streams_of[2], 1), 0, REL - 1).astype(jnp.int32),
        "edge_target": draw_edge_target(jax.random.fold_in(streams_of[14], 71), 0),
        "block_count": draw_block_count(jax.random.fold_in(streams_of[14], 71), 0),
        "send_list": place_ends(jax.random.randint(streams_of[5], (N_DOM, N_DOM, SLOT), 0, NODE_DEV), jax.random.fold_in(streams_of[5], 1), 0, NODE_DEV - 1).astype(jnp.int32),
        "bases_first": scatter_about(streams_of[6], (BASES, D, D), D ** -0.5, 0.375, ((1, 128),)),
        "self_first": scatter_about(streams_of[7], (D, D), D ** -0.5, 0.375, ((0, 128),)),
        "coef_first": scatter_about(streams_of[8], (REL, BASES), BASES ** -0.5, 1.0, (), jnp.float32),
        "bias_first": scatter_about(streams_of[9], (D,), 0.5, 3.0, (), jnp.float32),
        "bases_second": scatter_about(streams_of[10], (BASES, D, D), D ** -0.5, 0.375, ((1, 128),)),
        "self_second": scatter_about(streams_of[11], (D, D), D ** -0.5, 0.375, ((0, 128),)),
        "coef_second": scatter_about(streams_of[12], (REL, BASES), BASES ** -0.5, 1.0, (), jnp.float32),
        "bias_second": scatter_about(streams_of[13], (D,), 0.5, 3.0, (), jnp.float32),
    }


def compose_weights(coef, bases):
    mixed = jnp.einsum("rb,bij->rij", coef, bases.astype(jnp.float32), precision=lax.Precision.HIGHEST)
    return mixed.astype(jnp.bfloat16)


def relational_layer(inputs_now, edge_source, edge_relation, edge_target, block_count, send_list, mixed, self_weight, bias):
    owners = jnp.arange(N_DOM, dtype=jnp.int32)

    def one_part(part_index):
        received = inputs_now[owners[:, None], send_list[:, part_index, :]].reshape(-1, D)
        row_table = jnp.concatenate([inputs_now[part_index], received], axis=0)
        sources = edge_source[part_index].reshape(-1)
        relation_ids = edge_relation[part_index].reshape(-1)
        targets = edge_target[part_index].reshape(-1)
        block_ids = lax.broadcasted_iota(jnp.int32, (BLOCKS, EBLK), 0).reshape(-1)
        in_use = block_ids < block_count[part_index]
        messages = row_table[sources].astype(jnp.float32)
        segment = jnp.where(in_use, targets * REL + relation_ids, NODE_DEV * REL)
        degree = jax.ops.segment_sum(jnp.ones(segment.shape, jnp.float32), segment, NODE_DEV * REL + 1)[:NODE_DEV * REL]
        pooled = jax.ops.segment_sum(messages, segment, NODE_DEV * REL + 1)[:NODE_DEV * REL]
        averaged = (pooled / jnp.maximum(degree, 1.0)[:, None]).astype(jnp.bfloat16).reshape(NODE_DEV, REL, D)
        summed_all = jnp.dot(inputs_now[part_index], self_weight, preferred_element_type=jnp.float32) + bias
        for relation in range(REL):
            summed_all = summed_all + jnp.dot(averaged[:, relation, :], mixed[relation], preferred_element_type=jnp.float32)
        return summed_all

    return lax.map(one_part, owners)


def reference(features, edge_source, edge_relation, edge_target, block_count, send_list, bases_first, self_first, coef_first, bias_first, bases_second, self_second, coef_second, bias_second):
    inputs_now = features.reshape(N_DOM, NODE_DEV, D)
    mixed_first = compose_weights(coef_first, bases_first)
    first = relational_layer(inputs_now, edge_source, edge_relation, edge_target, block_count, send_list, mixed_first, self_first, bias_first)
    hidden = jnp.maximum(first, 0.0).astype(jnp.bfloat16)
    mixed_second = compose_weights(coef_second, bases_second)
    second = relational_layer(hidden, edge_source, edge_relation, edge_target, block_count, send_list, mixed_second, self_second, bias_second)
    return second.astype(jnp.bfloat16).reshape(N_DOM * NODE_DEV, D)
```

```python
import functools

import jax
import jax.numpy as jnp
from jax import lax
from jax.experimental import pallas as pl
from jax.experimental.pallas import tpu as pltpu
from jax.sharding import PartitionSpec as P

WIN = 16
LANES = 128
VMEM = pl.BlockSpec(memory_space=pltpu.VMEM)
SMEM = pl.BlockSpec(memory_space=pltpu.SMEM)
LIMIT = 60 * 1024 * 1024


def compose_weights(coef, bases):
    mixed = jnp.einsum(
        "rb,bij->rij", coef, bases.astype(jnp.float32), precision=lax.Precision.HIGHEST
    )
    return mixed.astype(jnp.bfloat16)


def layer_weights(bases, self_weight, coef):
    stacked = jnp.concatenate([compose_weights(coef, bases), self_weight[None]], axis=0)
    return lax.all_gather(stacked, "dom", axis=1, tiled=True)


def pick_rows(send_ref, rows_ref, out_ref):
    peers, slots = send_ref.shape
    nodes, width = rows_ref.shape
    group = 8

    def step(g, carry):
        ids = send_ref[pl.ds(pl.multiple_of(g * group, group), group), :]
        hot = (
            ids[:, :, None]
            == lax.broadcasted_iota(jnp.int32, (group, slots, nodes), 2)
        ).astype(jnp.float32).astype(jnp.bfloat16).reshape(group * slots, nodes)
        got = jnp.dot(hot, rows_ref[...], preferred_element_type=jnp.float32)
        out_ref[pl.ds(g * group, group)] = got.astype(jnp.bfloat16).reshape(group, slots, width)
        return carry

    lax.fori_loop(0, peers // group, step, 0)


def outgoing_rows(send_rows, rows):
    peers, slots = send_rows.shape
    return pl.pallas_call(
        pick_rows,
        out_shape=jax.ShapeDtypeStruct((peers, slots, rows.shape[1]), jnp.bfloat16),
        in_specs=[VMEM, VMEM],
        out_specs=VMEM,
        compiler_params=pltpu.CompilerParams(vmem_limit_bytes=LIMIT),
        name="outgoing_rows",
    )(send_rows, rows)


def layer_body(
    relu,
    count_ref,
    window_ref,
    source_ref,
    slot_ref,
    own_ref,
    recv_ref,
    weight_ref,
    bias_ref,
    out_ref,
    table,
    pooled,
    counts,
    stage_a,
    stage_b,
):
    nodes, width = own_ref.shape
    relations = weight_ref.shape[0] - 1
    block_width = slot_ref.shape[1]
    slots = WIN * relations
    chunk = 256

    def fill(src_ref, base):
        def step(i, carry):
            rows = src_ref[pl.ds(pl.multiple_of(i * chunk, chunk), chunk), :].astype(jnp.float32)
            at = pl.multiple_of(base + i * 2 * chunk, 2 * chunk)
            table[pl.ds(at, chunk, stride=2), :] = rows[:, :LANES]
            table[pl.ds(at + 1, chunk, stride=2), :] = rows[:, LANES:]
            return carry

        lax.fori_loop(0, src_ref.shape[0] // chunk, step, 0)

    fill(own_ref, 0)
    fill(recv_ref, 2 * nodes)

    def clear(i, carry):
        at = pl.multiple_of(i * slots, slots)
        pooled[pl.ds(at, slots), :] = jnp.zeros((slots, width), jnp.float32)
        counts[pl.ds(at, slots), :] = jnp.zeros((slots, LANES), jnp.float32)
        return carry

    lax.fori_loop(0, nodes // WIN, clear, 0)

    def gather(block, stage):
        for e in range(block_width):
            at = pl.multiple_of(source_ref[block, e], 2)
            stage[pl.ds(2 * e, 2), :] = table[pl.ds(at, 2), :]

    def pool(block, stage):
        hot = (
            slot_ref[pl.ds(block, 1), :]
            == lax.broadcasted_iota(jnp.int32, (slots, block_width), 0)
        ).astype(jnp.float32).astype(jnp.bfloat16)
        left = stage[pl.ds(0, block_width, stride=2), :].astype(jnp.bfloat16)
        right = stage[pl.ds(1, block_width, stride=2), :].astype(jnp.bfloat16)
        ones = jnp.ones((block_width, LANES), jnp.bfloat16)
        at = pl.multiple_of(window_ref[block] * slots, slots)
        rows = pl.ds(at, slots)
        pooled[rows, :LANES] += jnp.dot(hot, left, preferred_element_type=jnp.float32)
        pooled[rows, LANES:] += jnp.dot(hot, right, preferred_element_type=jnp.float32)
        counts[rows, :] += jnp.dot(hot, ones, preferred_element_type=jnp.float32)

    used = count_ref[0]

    def pair(i, carry):
        gather(2 * i, stage_a)
        pool(2 * i, stage_a)
        gather(2 * i + 1, stage_b)
        pool(2 * i + 1, stage_b)
        return carry

    lax.fori_loop(0, (used + 1) // 2, pair, 0)

    part = 256
    windows = part // WIN

    def finish(i, carry):
        at = pl.multiple_of(i * part, part)
        total = jnp.dot(
            own_ref[pl.ds(at, part), :], weight_ref[relations], preferred_element_type=jnp.float32
        ) + bias_ref[...]
        base = pl.multiple_of(i * windows * slots, windows * slots)
        sums = pooled[pl.ds(base, windows * slots), :].reshape(windows, relations, WIN, width)
        tally = counts[pl.ds(base, windows * slots), :].reshape(windows, relations, WIN, LANES)
        for r in range(relations):
            inverse = 1.0 / jnp.maximum(tally[:, r].reshape(part, LANES), 1.0)
            sums_r = sums[:, r].reshape(part, width)
            mean = jnp.concatenate(
                [sums_r[:, :LANES] * inverse, sums_r[:, LANES:] * inverse], axis=1
            ).astype(jnp.bfloat16)
            total = total + jnp.dot(mean, weight_ref[r], preferred_element_type=jnp.float32)
        if relu:
            total = jnp.maximum(total, 0.0)
        out_ref[pl.ds(at, part), :] = total.astype(jnp.bfloat16)
        return carry

    lax.fori_loop(0, nodes // part, finish, 0)


def relational_layer(relu, rows, received, count, windows, sources, slot_ids, weights, bias):
    nodes, width = rows.shape
    relations = weights.shape[0] - 1
    table_rows = 2 * (nodes + received.shape[0])
    return pl.pallas_call(
        functools.partial(layer_body, relu),
        out_shape=jax.ShapeDtypeStruct((nodes, width), jnp.bfloat16),
        in_specs=[SMEM, SMEM, SMEM, VMEM, VMEM, VMEM, VMEM, VMEM],
        out_specs=VMEM,
        scratch_shapes=[
            pltpu.VMEM((table_rows, LANES), jnp.float32),
            pltpu.VMEM((nodes * relations, width), jnp.float32),
            pltpu.VMEM((nodes * relations, LANES), jnp.float32),
            pltpu.VMEM((2 * LANES, LANES), jnp.float32),
            pltpu.VMEM((2 * LANES, LANES), jnp.float32),
        ],
        compiler_params=pltpu.CompilerParams(vmem_limit_bytes=LIMIT),
        name="relational_layer",
    )(count, windows, sources, slot_ids, rows, received, weights, bias.reshape(1, width))


def shards(
    features,
    edge_source,
    edge_relation,
    edge_target,
    block_count,
    send_list,
    bases_first,
    self_first,
    coef_first,
    bias_first,
    bases_second,
    self_second,
    coef_second,
    bias_second,
):
    sources = edge_source[0] * 2
    targets = edge_target[0]
    windows = targets[:, 0] // WIN
    blocks = targets.shape[0]
    in_use = lax.broadcasted_iota(jnp.int32, targets.shape, 0) < block_count[0]
    slot_ids = jnp.where(in_use, edge_relation[0] * WIN + targets % WIN, -1)
    send_rows = send_list[0]
    width = features.shape[1]

    def exchange(rows):
        out = outgoing_rows(send_rows, rows)
        incoming = lax.all_to_all(out, "dom", split_axis=0, concat_axis=0, tiled=True)
        return incoming.reshape(-1, width)

    first_weights = layer_weights(bases_first, self_first, coef_first)
    second_weights = layer_weights(bases_second, self_second, coef_second)
    hidden = relational_layer(
        True, features, exchange(features), block_count, windows, sources, slot_ids,
        first_weights, bias_first,
    )
    return relational_layer(
        False, hidden, exchange(hidden), block_count, windows, sources, slot_ids,
        second_weights, bias_second,
    )


def solution(mesh):
    placed = (
        P("dom", None),
        P("dom", None, None),
        P("dom", None, None),
        P("dom", None, None),
        P("dom"),
        P("dom", None, None),
        P(None, "dom", None),
        P("dom", None),
        P(),
        P(),
        P(None, "dom", None),
        P("dom", None),
        P(),
        P(),
    )
    return jax.shard_map(
        shards, mesh=mesh, in_specs=placed, out_specs=P("dom", None), check_vma=False
    )
```

```python
import functools

import jax
import jax.numpy as jnp
from jax import lax
from jax.experimental import pallas as pl
from jax.experimental.pallas import tpu as pltpu
from jax.sharding import PartitionSpec as P

WIN = 16
LANES = 128
VMEM = pl.BlockSpec(memory_space=pltpu.VMEM)
SMEM = pl.BlockSpec(memory_space=pltpu.SMEM)
LIMIT = 60 * 1024 * 1024


def compose_weights(coef, bases):
    mixed = jnp.einsum(
        "rb,bij->rij", coef, bases.astype(jnp.float32), precision=lax.Precision.HIGHEST
    )
    return mixed.astype(jnp.bfloat16)


def weight_part(bases, self_weight, coef):
    stacked = jnp.concatenate([compose_weights(coef, bases), self_weight[None]], axis=0)
    matrices, pair, width = stacked.shape
    split = stacked.reshape(matrices, pair, width // LANES, LANES).transpose(0, 2, 1, 3)
    return split[:, :, None]


def pick_rows(send_ref, rows_ref, out_ref):
    peers, slots = send_ref.shape
    nodes, width = rows_ref.shape
    group = 8

    def step(g, carry):
        ids = send_ref[pl.ds(pl.multiple_of(g * group, group), group), :]
        hot = (
            ids[:, :, None]
            == lax.broadcasted_iota(jnp.int32, (group, slots, nodes), 2)
        ).astype(jnp.float32).astype(jnp.bfloat16).reshape(group * slots, nodes)
        got = jnp.dot(hot, rows_ref[...], preferred_element_type=jnp.float32)
        out_ref[pl.ds(g * group, group)] = got.astype(jnp.bfloat16).reshape(group, slots, width)
        return carry

    lax.fori_loop(0, peers // group, step, 0)


def outgoing_rows(send_rows, rows):
    peers, slots = send_rows.shape
    return pl.pallas_call(
        pick_rows,
        out_shape=jax.ShapeDtypeStruct((peers, slots, rows.shape[1]), jnp.bfloat16),
        in_specs=[VMEM, VMEM],
        out_specs=VMEM,
        compiler_params=pltpu.CompilerParams(vmem_limit_bytes=LIMIT),
        name="outgoing_rows",
    )(send_rows, rows)


MESH = pl.DeviceIdType.MESH
ANY = pl.BlockSpec(memory_space=pl.ANY)
BATCHES = (6, 6, 14, 14, 28, 28, 31)


def greet(me, count):
    barrier = pltpu.get_barrier_semaphore()

    def signal(k, carry):
        pl.semaphore_signal(
            barrier, inc=1, device_id=(lax.rem(me + k, count),), device_id_type=MESH
        )
        return carry

    lax.fori_loop(1, count, signal, 0)
    pl.semaphore_wait(barrier, count - 1)


def send_blocks(me, count, first, last, out_ref, in_ref, send_sem, recv_sem):
    def send(k, carry):
        to = lax.rem(me + lax.rem(k * 37, count), count)
        pltpu.make_async_remote_copy(
            src_ref=out_ref.at[to],
            dst_ref=in_ref.at[me],
            send_sem=send_sem,
            recv_sem=recv_sem,
            device_id=(to,),
            device_id_type=MESH,
        ).start()
        return carry

    lax.fori_loop(first, last, send, 0)


def drain_blocks(count, out_ref, in_ref, send_sem, recv_sem):
    some = pl.ds(0, count - 1)
    pltpu.make_async_copy(in_ref.at[some], in_ref.at[some], recv_sem).wait()
    pltpu.make_async_copy(out_ref.at[some], out_ref.at[some], send_sem).wait()


def exchange_body(count, out_ref, in_ref, send_sem, recv_sem, own_sem):
    me = lax.axis_index("dom")
    own = pltpu.make_async_copy(out_ref.at[me], in_ref.at[me], own_sem)
    own.start()
    greet(me, count)
    send_blocks(me, count, 1, count, out_ref, in_ref, send_sem, recv_sem)
    own.wait()
    drain_blocks(count, out_ref, in_ref, send_sem, recv_sem)


def exchange_gather_body(
    count,
    out_ref,
    part_ref,
    in_ref,
    full_ref,
    send_sem,
    recv_sem,
    own_sem,
    part_sem,
    hop_send,
    hop_recv,
):
    me = lax.axis_index("dom")
    core = lax.rem(me, 2)
    other = me + 1 - 2 * core
    own = pltpu.make_async_copy(out_ref.at[me], in_ref.at[me], own_sem)
    own.start()
    mine = pltpu.make_async_copy(
        part_ref.at[core], full_ref.at[core, :, :, pl.ds(me, 1)], part_sem
    )
    mine.start()
    greet(me, count)

    started = []

    def hop(index, src, dst, to):
        copy = pltpu.make_async_remote_copy(
            src_ref=src,
            dst_ref=dst,
            send_sem=hop_send.at[index],
            recv_sem=hop_recv.at[index],
            device_id=(to,),
            device_id_type=MESH,
        )
        copy.start()
        started.append(copy)
        return copy

    sent = 1

    def batch(stage):
        nonlocal sent
        last = sent + BATCHES[stage]
        send_blocks(me, count, sent, last, out_ref, in_ref, send_sem, recv_sem)
        sent = last

    pair = hop(
        0, part_ref.at[1 - core], full_ref.at[1 - core, :, :, pl.ds(me, 1)], other
    )
    batch(0)
    mine.wait()
    pair.wait_recv()
    stage = 1
    index = 1
    for step in (2, 8, 32):
        place = lax.rem(me // step, 4)
        base = (me // (4 * step)) * (4 * step)
        inner = lax.rem(me, step)

        def at(p, half=None):
            p = lax.rem(p + 8, 4)
            size = step if half is None else step // 2
            start = base + p * step + (0 if half is None else half * size)
            return full_ref.at[core, :, :, pl.ds(start, size)]

        def device(p):
            return base + lax.rem(p + 8, 4) * step + inner

        up = hop(index, at(place), at(place), device(place + 1))
        down = hop(index + 1, at(place), at(place), device(place - 1))
        batch(stage)
        up.wait_recv()
        down.wait_recv()
        far_up = hop(index + 2, at(place - 1, 0), at(place - 1, 0), device(place + 1))
        far_down = hop(index + 3, at(place + 1, 1), at(place + 1, 1), device(place - 1))
        batch(stage + 1)
        far_up.wait_recv()
        far_down.wait_recv()
        stage += 2
        index += 4
    last = hop(index, full_ref.at[core], full_ref.at[core], other)
    last.wait_recv()
    for copy in started:
        copy.wait_send()
    own.wait()
    drain_blocks(count, out_ref, in_ref, send_sem, recv_sem)


def exchange(out, count):
    return pl.pallas_call(
        functools.partial(exchange_body, count),
        out_shape=jax.ShapeDtypeStruct(out.shape, out.dtype),
        in_specs=[VMEM],
        out_specs=VMEM,
        scratch_shapes=[pltpu.SemaphoreType.DMA] * 3,
        compiler_params=pltpu.CompilerParams(
            collective_id=1, has_side_effects=True, vmem_limit_bytes=LIMIT
        ),
        name="exchange",
    )(out)


def exchange_gather(out, part, count):
    layers, matrices, halves, _, pair, lanes = part.shape
    return pl.pallas_call(
        functools.partial(exchange_gather_body, count),
        out_shape=(
            jax.ShapeDtypeStruct(out.shape, out.dtype),
            jax.ShapeDtypeStruct((layers, matrices, halves, count, pair, lanes), part.dtype),
        ),
        in_specs=[VMEM, VMEM],
        out_specs=(VMEM, VMEM),
        scratch_shapes=[pltpu.SemaphoreType.DMA] * 4
        + [pltpu.SemaphoreType.DMA((14,)), pltpu.SemaphoreType.DMA((14,))],
        compiler_params=pltpu.CompilerParams(
            collective_id=0, has_side_effects=True, vmem_limit_bytes=LIMIT
        ),
        name="exchange_gather",
    )(out, part)


def layer_body(
    relu,
    count_ref,
    window_ref,
    source_ref,
    slot_ref,
    own_ref,
    recv_ref,
    weight_ref,
    bias_ref,
    out_ref,
    table,
    pooled,
    counts,
    stage_a,
    stage_b,
):
    nodes, width = own_ref.shape
    relations = weight_ref.shape[0] - 1
    block_width = slot_ref.shape[1]
    slots = WIN * relations
    chunk = 256

    def fill(src_ref, base):
        def step(i, carry):
            rows = src_ref[pl.ds(pl.multiple_of(i * chunk, chunk), chunk), :].astype(jnp.float32)
            at = pl.multiple_of(base + i * 2 * chunk, 2 * chunk)
            table[pl.ds(at, chunk, stride=2), :] = rows[:, :LANES]
            table[pl.ds(at + 1, chunk, stride=2), :] = rows[:, LANES:]
            return carry

        lax.fori_loop(0, src_ref.shape[0] // chunk, step, 0)

    fill(own_ref, 0)
    fill(recv_ref, 2 * nodes)

    def clear(i, carry):
        at = pl.multiple_of(i * slots, slots)
        pooled[pl.ds(at, slots), :] = jnp.zeros((slots, width), jnp.float32)
        counts[pl.ds(at, slots), :] = jnp.zeros((slots, LANES), jnp.float32)
        return carry

    lax.fori_loop(0, nodes // WIN, clear, 0)

    def gather(block, stage):
        for e in range(block_width):
            at = pl.multiple_of(source_ref[block, e], 2)
            stage[pl.ds(2 * e, 2), :] = table[pl.ds(at, 2), :]

    def pool(block, stage):
        hot = (
            slot_ref[pl.ds(block, 1), :]
            == lax.broadcasted_iota(jnp.int32, (slots, block_width), 0)
        ).astype(jnp.float32).astype(jnp.bfloat16)
        left = stage[pl.ds(0, block_width, stride=2), :].astype(jnp.bfloat16)
        right = stage[pl.ds(1, block_width, stride=2), :].astype(jnp.bfloat16)
        ones = jnp.ones((block_width, LANES), jnp.bfloat16)
        at = pl.multiple_of(window_ref[block] * slots, slots)
        rows = pl.ds(at, slots)
        pooled[rows, :LANES] += jnp.dot(hot, left, preferred_element_type=jnp.float32)
        pooled[rows, LANES:] += jnp.dot(hot, right, preferred_element_type=jnp.float32)
        counts[rows, :] += jnp.dot(hot, ones, preferred_element_type=jnp.float32)

    used = count_ref[0]

    def pair(i, carry):
        gather(2 * i, stage_a)
        pool(2 * i, stage_a)
        gather(2 * i + 1, stage_b)
        pool(2 * i + 1, stage_b)
        return carry

    lax.fori_loop(0, (used + 1) // 2, pair, 0)

    part = 256
    windows = part // WIN

    def finish(i, carry):
        at = pl.multiple_of(i * part, part)
        own = own_ref[pl.ds(at, part), :]
        totals = [
            jnp.dot(own, weight_ref[relations, h], preferred_element_type=jnp.float32)
            + bias_ref[:, h * LANES : (h + 1) * LANES]
            for h in range(2)
        ]
        base = pl.multiple_of(i * windows * slots, windows * slots)
        sums = pooled[pl.ds(base, windows * slots), :].reshape(windows, relations, WIN, width)
        tally = counts[pl.ds(base, windows * slots), :].reshape(windows, relations, WIN, LANES)
        for r in range(relations):
            inverse = 1.0 / jnp.maximum(tally[:, r].reshape(part, LANES), 1.0)
            sums_r = sums[:, r].reshape(part, width)
            mean = jnp.concatenate(
                [sums_r[:, :LANES] * inverse, sums_r[:, LANES:] * inverse], axis=1
            ).astype(jnp.bfloat16)
            totals = [
                totals[h] + jnp.dot(mean, weight_ref[r, h], preferred_element_type=jnp.float32)
                for h in range(2)
            ]
        total = jnp.concatenate(totals, axis=1)
        if relu:
            total = jnp.maximum(total, 0.0)
        out_ref[pl.ds(at, part), :] = total.astype(jnp.bfloat16)
        return carry

    lax.fori_loop(0, nodes // part, finish, 0)


def relational_layer(relu, rows, received, count, windows, sources, slot_ids, weights, bias):
    nodes, width = rows.shape
    relations = weights.shape[0] - 1
    table_rows = 2 * (nodes + received.shape[0])
    return pl.pallas_call(
        functools.partial(layer_body, relu),
        out_shape=jax.ShapeDtypeStruct((nodes, width), jnp.bfloat16),
        in_specs=[SMEM, SMEM, SMEM, VMEM, VMEM, VMEM, VMEM, VMEM],
        out_specs=VMEM,
        scratch_shapes=[
            pltpu.VMEM((table_rows, LANES), jnp.float32),
            pltpu.VMEM((nodes * relations, width), jnp.float32),
            pltpu.VMEM((nodes * relations, LANES), jnp.float32),
            pltpu.VMEM((2 * LANES, LANES), jnp.float32),
            pltpu.VMEM((2 * LANES, LANES), jnp.float32),
        ],
        compiler_params=pltpu.CompilerParams(vmem_limit_bytes=LIMIT),
        name="relational_layer",
    )(count, windows, sources, slot_ids, rows, received, weights, bias.reshape(1, width))


def shards(
    features,
    edge_source,
    edge_relation,
    edge_target,
    block_count,
    send_list,
    bases_first,
    self_first,
    coef_first,
    bias_first,
    bases_second,
    self_second,
    coef_second,
    bias_second,
):
    sources = edge_source[0] * 2
    targets = edge_target[0]
    windows = targets[:, 0] // WIN
    blocks = targets.shape[0]
    in_use = lax.broadcasted_iota(jnp.int32, targets.shape, 0) < block_count[0]
    slot_ids = jnp.where(in_use, edge_relation[0] * WIN + targets % WIN, -1)
    send_rows = send_list[0]
    width = features.shape[1]

    part = jnp.stack(
        [
            weight_part(bases_first, self_first, coef_first),
            weight_part(bases_second, self_second, coef_second),
        ]
    )
    count = send_rows.shape[0]
    received, full = exchange_gather(outgoing_rows(send_rows, features), part, count)
    full = full.reshape(full.shape[:3] + (width, LANES))
    hidden = relational_layer(
        True, features, received.reshape(-1, width), block_count, windows, sources, slot_ids,
        full[0], bias_first,
    )
    received = exchange(outgoing_rows(send_rows, hidden), count)
    return relational_layer(
        False, hidden, received.reshape(-1, width), block_count, windows, sources, slot_ids,
        full[1], bias_second,
    )


def solution(mesh):
    placed = (
        P("dom", None),
        P("dom", None, None),
        P("dom", None, None),
        P("dom", None, None),
        P("dom"),
        P("dom", None, None),
        P(None, "dom", None),
        P("dom", None),
        P(),
        P(),
        P(None, "dom", None),
        P("dom", None),
        P(),
        P(),
    )
    return jax.shard_map(
        shards, mesh=mesh, in_specs=placed, out_specs=P("dom", None), check_vma=False
    )
```

```python
import functools

import jax
import jax.numpy as jnp
from jax import lax
from jax.experimental import pallas as pl
from jax.experimental.pallas import tpu as pltpu
from jax.sharding import PartitionSpec as P

WIN = 16
LANES = 128
VMEM = pl.BlockSpec(memory_space=pltpu.VMEM)
SMEM = pl.BlockSpec(memory_space=pltpu.SMEM)
LIMIT = 60 * 1024 * 1024


def compose_weights(coef, bases):
    mixed = jnp.einsum(
        "rb,bij->rij", coef, bases.astype(jnp.float32), precision=lax.Precision.HIGHEST
    )
    return mixed.astype(jnp.bfloat16)


def weight_part(bases, self_weight, coef):
    stacked = jnp.concatenate([compose_weights(coef, bases), self_weight[None]], axis=0)
    matrices, pair, width = stacked.shape
    split = stacked.reshape(matrices, pair, width // LANES, LANES).transpose(0, 2, 1, 3)
    return split


MESH = pl.DeviceIdType.MESH
ANY = pl.BlockSpec(memory_space=pl.ANY)
GROUP = 8
FIRST_GROUPS = 4


def rows_of_group(group, send_ref, rows_ref, out_ref):
    slots = send_ref.shape[1]
    nodes, width = rows_ref.shape
    ids = send_ref[pl.ds(pl.multiple_of(group * GROUP, GROUP), GROUP), :]
    hot = (
        (ids[:, :, None] == lax.broadcasted_iota(jnp.int32, (GROUP, slots, nodes), 2))
        .astype(jnp.float32)
        .astype(jnp.bfloat16)
        .reshape(GROUP * slots, nodes)
    )
    got = jnp.dot(hot, rows_ref[...], preferred_element_type=jnp.float32)
    out_ref[pl.ds(group * GROUP, GROUP)] = got.astype(jnp.bfloat16).reshape(GROUP, slots, width)


def remote(src, dst, send_sem, recv_sem, to):
    return pltpu.make_async_remote_copy(
        src_ref=src,
        dst_ref=dst,
        send_sem=send_sem,
        recv_sem=recv_sem,
        device_id=(to,),
        device_id_type=MESH,
    )


def exchange_body(count, with_weights, *refs):
    if with_weights:
        (send_ref, rows_ref, part_ref, in_ref, full_ref, out_ref, send_sem, recv_sem,
         plane_send, plane_recv, far_send, far_recv, core_send, core_recv) = refs
    else:
        send_ref, rows_ref, in_ref, out_ref, send_sem, recv_sem = refs
    me = lax.axis_index("dom")
    groups = count // GROUP
    barrier = pltpu.get_barrier_semaphore()

    def signal(k, carry):
        pl.semaphore_signal(
            barrier, inc=1, device_id=(lax.rem(me + k, count),), device_id_type=MESH
        )
        return carry

    lax.fori_loop(1, count, signal, 0)

    def group_at(t):
        return lax.rem(me // GROUP + 5 * t, groups)

    def compute(t):
        rows_of_group(group_at(t), send_ref, rows_ref, out_ref)

    def send(t, first):
        for i in range(first, GROUP):
            to = group_at(t) * GROUP + lax.rem(me + i, GROUP)
            remote(out_ref.at[to], in_ref.at[me], send_sem, recv_sem, to).start()

    def step(t, carry):
        compute(t + 1)
        send(t, 0)
        return carry

    compute(0)
    compute(1)
    pl.semaphore_wait(barrier, count - 1)
    if with_weights:
        core = lax.rem(me, 2)
        x = lax.rem(me // 2, 4)
        y = lax.rem(me // 8, 4)
        z = me // 32
        pair = lax.rem(me, 8)
        mine = pltpu.make_async_copy(
            part_ref.at[core], full_ref.at[core, :, :, z, y, pair], plane_recv
        )
        mine.start()

        def spread(layer):
            def one(k, carry):
                column = lax.rem(x + k, 4)
                if layer == 0:
                    line = (z * 4 + lax.rem(y + k // 4, 4)) * 4
                else:
                    line = (lax.rem(z + k // 4, 4) * 4 + y) * 4
                remote(
                    part_ref.at[layer],
                    full_ref.at[layer, :, :, z, y, pair],
                    plane_send.at[jnp.where(core == layer, 0, 1)],
                    plane_recv,
                    (line + column) * 2 + layer,
                ).start()
                return carry

            lax.fori_loop(jnp.where(core == layer, 1, 0), 16, one, 0)

        spread(0)
        spread(1)
    send(0, 1)
    if not with_weights:
        lax.fori_loop(1, groups - 1, step, 0)
    else:
        lax.fori_loop(1, FIRST_GROUPS, step, 0)
        arrived = full_ref.at[0, :, :, 0]
        pltpu.make_async_copy(arrived, arrived, plane_recv).wait()

        def far(layer):
            copies = []
            for k in (1, 3, 2):
                if layer == 0:
                    slab = full_ref.at[0, :, :, z]
                    to = lax.rem(me + 32 * k, count)
                else:
                    slab = full_ref.at[1, :, :, :, y]
                    to = z * 32 + lax.rem(y + k, 4) * 8 + pair
                copies.append(remote(slab, slab, far_send.at[k], far_recv.at[k], to))
            return copies

        for layer in range(2):
            @pl.when(core == layer)
            def _():
                for copy in far(layer):
                    copy.start()

        lax.fori_loop(FIRST_GROUPS, groups - 1, step, 0)
    send(groups - 1, 0)
    if with_weights:
        for layer in range(2):
            @pl.when(core == layer)
            def _():
                for copy in far(layer):
                    copy.wait()
        across = remote(
            full_ref.at[core], full_ref.at[core], core_send, core_recv, me + 1 - 2 * core
        )
        across.start()
        across.wait()
        gone = full_ref.at[0, :, :, 0:3, 0, 0:5]
        pltpu.make_async_copy(gone, gone, plane_send.at[0]).wait()
        gone = full_ref.at[0, :, :, 0:2, 0]
        pltpu.make_async_copy(gone, gone, plane_send.at[1]).wait()
    some = pl.ds(0, count - 1)
    pltpu.make_async_copy(in_ref.at[some], in_ref.at[some], recv_sem).wait()
    pltpu.make_async_copy(out_ref.at[some], out_ref.at[some], send_sem).wait()


def exchange(send_rows, rows, part=None):
    count, slots = send_rows.shape
    block = (count, slots, rows.shape[1])
    out_shape = [jax.ShapeDtypeStruct(block, rows.dtype)]
    inputs = [send_rows, rows]
    sems = [pltpu.SemaphoreType.DMA] * 2
    if part is not None:
        layers, matrices, halves, pair, lanes = part.shape
        inputs.append(part)
        out_shape.append(
            jax.ShapeDtypeStruct((layers, matrices, halves, 4, 4, 8, pair, lanes), part.dtype)
        )
        sems += [pltpu.SemaphoreType.DMA((2,)), pltpu.SemaphoreType.DMA]
        sems += [pltpu.SemaphoreType.DMA((4,))] * 2 + [pltpu.SemaphoreType.DMA] * 2
    return pl.pallas_call(
        functools.partial(exchange_body, count, part is not None),
        out_shape=out_shape,
        in_specs=[VMEM] * len(inputs),
        out_specs=[ANY] * len(out_shape),
        scratch_shapes=[pltpu.VMEM(block, rows.dtype)] + sems,
        compiler_params=pltpu.CompilerParams(
            collective_id=0 if part is not None else 1,
            has_side_effects=True,
            vmem_limit_bytes=LIMIT,
        ),
        name="exchange" if part is None else "exchange_weights",
    )(*inputs)


def layer_body(
    relu,
    layer,
    count_ref,
    window_ref,
    source_ref,
    target_ref,
    relation_ref,
    own_hbm,
    recv_hbm,
    weight_hbm,
    bias_ref,
    out_ref,
    table,
    pooled,
    counts,
    stage_a,
    own_ref,
    recv_ref,
    weight_ref,
    own_sem,
    recv_sem,
    weight_sem,
):
    nodes, width = own_ref.shape
    relations = weight_ref.shape[0] - 1
    blocks, block_width = target_ref.shape
    slots = WIN * relations
    chunk = 256
    pieces = recv_sem.shape[0]
    piece = recv_ref.shape[0] // pieces

    own_copy = pltpu.make_async_copy(own_hbm, own_ref, own_sem)
    own_copy.start()
    recv_copies = []
    for p in range(pieces):
        rows = pl.ds(p * piece, piece)
        copy = pltpu.make_async_copy(recv_hbm.at[rows], recv_ref.at[rows], recv_sem.at[p])
        copy.start()
        recv_copies.append(copy)
    weight_copy = pltpu.make_async_copy(weight_hbm.at[layer], weight_ref, weight_sem)
    weight_copy.start()

    def clear(i, carry):
        at = pl.multiple_of(i * slots, slots)
        pooled[pl.ds(at, slots), :] = jnp.zeros((slots, width), jnp.float32)
        counts[pl.ds(at, slots), :] = jnp.zeros((slots, LANES), jnp.float32)
        return carry

    lax.fori_loop(0, nodes // WIN, clear, 0)

    def fill(src_ref, first, last, base):
        def step(i, carry):
            rows = src_ref[pl.ds(pl.multiple_of(i * chunk, chunk), chunk), :].astype(jnp.float32)
            at = pl.multiple_of(base + i * 2 * chunk, 2 * chunk)
            table[pl.ds(at, chunk, stride=2), :] = rows[:, :LANES]
            table[pl.ds(at + 1, chunk, stride=2), :] = rows[:, LANES:]
            return carry

        lax.fori_loop(first, last, step, 0)

    own_copy.wait()
    fill(own_ref, 0, nodes // chunk, 0)
    for p in range(pieces):
        recv_copies[p].wait()
        fill(recv_ref, p * piece // chunk, (p + 1) * piece // chunk, 2 * nodes)

    used = count_ref[0]

    def gather(pair, stage):
        for h in range(2):
            row = source_ref.at[2 * pair + h]
            for e in range(block_width):
                at = pl.multiple_of(row[e], 2)
                stage[pl.ds(2 * (h * block_width + e), 2), :] = table[pl.ds(at, 2), :]

    def pool(pair, stage):
        ids = []
        for h in range(2):
            row = pl.ds(2 * pair + h, 1)
            shift = jnp.where(2 * pair + h < used, h * slots, 2 * slots)
            ids.append(relation_ref[row, :] * WIN + lax.rem(target_ref[row, :], WIN) + shift)
        both = jnp.concatenate(ids, axis=1)
        hot = (
            both == lax.broadcasted_iota(jnp.int32, (2 * slots, 2 * block_width), 0)
        ).astype(jnp.float32).astype(jnp.bfloat16)
        edges = 2 * block_width
        data = jnp.concatenate(
            [
                stage[pl.ds(0, edges, stride=2), :].astype(jnp.bfloat16),
                stage[pl.ds(1, edges, stride=2), :].astype(jnp.bfloat16),
                jnp.ones((edges, LANES), jnp.bfloat16),
            ],
            axis=1,
        )
        got = jnp.dot(hot, data, preferred_element_type=jnp.float32)
        for h in range(2):
            at = pl.multiple_of(window_ref[2 * pair + h] * slots, slots)
            rows = pl.ds(at, slots)
            pooled[rows, :] += got[h * slots : (h + 1) * slots, :width]
            counts[rows, :] += got[h * slots : (h + 1) * slots, width:]

    gather(0, stage_a)

    def pair_step(i, carry):
        pool(i, stage_a)
        gather(jnp.minimum(i + 1, blocks // 2 - 1), stage_a)
        return carry

    lax.fori_loop(0, (used + 1) // 2, pair_step, 0)

    weight_copy.wait()
    part = 256
    windows = part // WIN

    def finish(i, carry):
        at = pl.multiple_of(i * part, part)
        own = own_ref[pl.ds(at, part), :]
        totals = [
            jnp.dot(own, weight_ref[relations, h], preferred_element_type=jnp.float32)
            + bias_ref[:, h * LANES : (h + 1) * LANES]
            for h in range(2)
        ]
        base = pl.multiple_of(i * windows * slots, windows * slots)
        sums = pooled[pl.ds(base, windows * slots), :].reshape(windows, relations, WIN, width)
        tally = counts[pl.ds(base, windows * slots), :].reshape(windows, relations, WIN, LANES)
        for r in range(relations):
            inverse = 1.0 / jnp.maximum(tally[:, r].reshape(part, LANES), 1.0)
            sums_r = sums[:, r].reshape(part, width)
            mean = jnp.concatenate(
                [sums_r[:, :LANES] * inverse, sums_r[:, LANES:] * inverse], axis=1
            ).astype(jnp.bfloat16)
            totals = [
                totals[h] + jnp.dot(mean, weight_ref[r, h], preferred_element_type=jnp.float32)
                for h in range(2)
            ]
        total = jnp.concatenate(totals, axis=1)
        if relu:
            total = jnp.maximum(total, 0.0)
        out_ref[pl.ds(at, part), :] = total.astype(jnp.bfloat16)
        return carry

    lax.fori_loop(0, nodes // part, finish, 0)


def relational_layer(
    layer, rows, received, count, windows, sources, targets, relation_ids, weights, bias
):
    nodes, width = rows.shape
    relations = weights.shape[1] - 1
    table_rows = 2 * (nodes + received.shape[0])
    pieces = 4
    return pl.pallas_call(
        functools.partial(layer_body, layer == 0, layer),
        out_shape=jax.ShapeDtypeStruct((nodes, width), jnp.bfloat16),
        in_specs=[SMEM, SMEM, SMEM, VMEM, VMEM, ANY, ANY, ANY, VMEM],
        out_specs=VMEM,
        scratch_shapes=[
            pltpu.VMEM((table_rows, LANES), jnp.float32),
            pltpu.VMEM((nodes * relations, width), jnp.float32),
            pltpu.VMEM((nodes * relations, LANES), jnp.float32),
            pltpu.VMEM((4 * LANES, LANES), jnp.float32),
            pltpu.VMEM(rows.shape, rows.dtype),
            pltpu.VMEM(received.shape, received.dtype),
            pltpu.VMEM(weights.shape[1:], weights.dtype),
            pltpu.SemaphoreType.DMA,
            pltpu.SemaphoreType.DMA((pieces,)),
            pltpu.SemaphoreType.DMA,
        ],
        compiler_params=pltpu.CompilerParams(vmem_limit_bytes=LIMIT),
        name="relational_layer",
    )(
        count, windows, sources, targets, relation_ids, rows, received, weights,
        bias.reshape(1, width),
    )


def shards(
    features,
    edge_source,
    edge_relation,
    edge_target,
    block_count,
    send_list,
    bases_first,
    self_first,
    coef_first,
    bias_first,
    bases_second,
    self_second,
    coef_second,
    bias_second,
):
    sources = edge_source[0] * 2
    targets = edge_target[0]
    windows = targets[:, 0] // WIN
    send_rows = send_list[0]
    width = features.shape[1]

    part = jnp.stack(
        [
            weight_part(bases_first, self_first, coef_first),
            weight_part(bases_second, self_second, coef_second),
        ]
    )
    received, full = exchange(send_rows, features, part)
    full = full.reshape(full.shape[:3] + (width, LANES))
    hidden = relational_layer(
        0, features, received.reshape(-1, width), block_count, windows, sources, targets,
        edge_relation[0], full, bias_first,
    )
    (received,) = exchange(send_rows, hidden)
    return relational_layer(
        1, hidden, received.reshape(-1, width), block_count, windows, sources, targets,
        edge_relation[0], full, bias_second,
    )


def solution(mesh):
    placed = (
        P("dom", None),
        P("dom", None, None),
        P("dom", None, None),
        P("dom", None, None),
        P("dom"),
        P("dom", None, None),
        P(None, "dom", None),
        P("dom", None),
        P(),
        P(),
        P(None, "dom", None),
        P("dom", None),
        P(),
        P(),
    )
    return jax.shard_map(
        shards, mesh=mesh, in_specs=placed, out_specs=P("dom", None), check_vma=False
    )
```

```python
import functools

import jax
import jax.numpy as jnp
from jax import lax
from jax.experimental import pallas as pl
from jax.experimental.pallas import tpu as pltpu
from jax.sharding import PartitionSpec as P

WIN = 16
LANES = 128
VMEM = pl.BlockSpec(memory_space=pltpu.VMEM)
SMEM = pl.BlockSpec(memory_space=pltpu.SMEM)
LIMIT = 60 * 1024 * 1024


def mix_weights(layer, coef_ref, bases_ref, self_ref, part_ref):
    relations = coef_ref.shape[0]
    rows = []
    for i in range(2):
        bases = bases_ref[:, i, :].astype(jnp.float32)
        rows.append(
            jnp.dot(
                coef_ref[...],
                bases,
                precision=lax.Precision.HIGHEST,
                preferred_element_type=jnp.float32,
            )
        )
    for h in range(2):
        lanes = slice(h * LANES, (h + 1) * LANES)
        for r in range(relations):
            both = jnp.concatenate([row[r : r + 1, lanes] for row in rows], axis=0)
            part_ref[layer, r, h] = both.astype(jnp.bfloat16)
        part_ref[layer, relations, h] = self_ref[:, lanes]


MESH = pl.DeviceIdType.MESH
ANY = pl.BlockSpec(memory_space=pl.ANY)
GROUP = 8
FIRST_GROUPS = 4


def rows_of_group(group, send_ref, rows_ref, out_ref):
    slots = send_ref.shape[1]
    nodes, width = rows_ref.shape
    ids = send_ref[pl.ds(pl.multiple_of(group * GROUP, GROUP), GROUP), :]
    hot = (
        (ids[:, :, None] == lax.broadcasted_iota(jnp.int32, (GROUP, slots, nodes), 2))
        .astype(jnp.float32)
        .astype(jnp.bfloat16)
        .reshape(GROUP * slots, nodes)
    )
    got = jnp.dot(hot, rows_ref[...], preferred_element_type=jnp.float32)
    out_ref[pl.ds(group * GROUP, GROUP)] = got.astype(jnp.bfloat16).reshape(GROUP, slots, width)


def remote(src, dst, send_sem, recv_sem, to):
    return pltpu.make_async_remote_copy(
        src_ref=src,
        dst_ref=dst,
        send_sem=send_sem,
        recv_sem=recv_sem,
        device_id=(to,),
        device_id_type=MESH,
    )


def exchange_body(count, with_weights, *refs):
    if with_weights:
        (turned_ref, rows_ref, coef_a, bases_a, self_a, coef_b, bases_b, self_b,
         in_ref, full_ref, out_ref, send_ref, part_ref, send_sem, recv_sem,
         plane_send, plane_recv, far_send, far_recv, core_send, core_recv) = refs
    else:
        turned_ref, rows_ref, in_ref, out_ref, send_ref, send_sem, recv_sem = refs
    me = lax.axis_index("dom")
    groups = count // GROUP
    barrier = pltpu.get_barrier_semaphore()

    def signal(k, carry):
        pl.semaphore_signal(
            barrier, inc=1, device_id=(lax.rem(me + k, count),), device_id_type=MESH
        )
        return carry

    lax.fori_loop(1, count, signal, 0)

    def group_at(t):
        return lax.rem(me // GROUP + 5 * t, groups)

    def compute(t):
        rows_of_group(group_at(t), send_ref, rows_ref, out_ref)

    def send(t, first):
        for i in range(first, GROUP):
            to = group_at(t) * GROUP + lax.rem(me + i, GROUP)
            remote(out_ref.at[to], in_ref.at[me], send_sem, recv_sem, to).start()

    def step(t, carry):
        compute(t + 1)
        send(t, 0)
        return carry

    send_ref[...] = turned_ref[...].T
    if with_weights:
        mix_weights(0, coef_a, bases_a, self_a, part_ref)
        mix_weights(1, coef_b, bases_b, self_b, part_ref)
    compute(0)
    compute(1)
    pl.semaphore_wait(barrier, count - 1)
    if with_weights:
        core = lax.rem(me, 2)
        x = lax.rem(me // 2, 4)
        y = lax.rem(me // 8, 4)
        z = me // 32
        pair = lax.rem(me, 8)
        mine = pltpu.make_async_copy(
            part_ref.at[core], full_ref.at[core, :, :, z, y, pair], plane_recv
        )
        mine.start()

        def spread(layer):
            def one(k, carry):
                column = lax.rem(x + k, 4)
                if layer == 0:
                    line = (z * 4 + lax.rem(y + k // 4, 4)) * 4
                else:
                    line = (lax.rem(z + k // 4, 4) * 4 + y) * 4
                remote(
                    part_ref.at[layer],
                    full_ref.at[layer, :, :, z, y, pair],
                    plane_send.at[jnp.where(core == layer, 0, 1)],
                    plane_recv,
                    (line + column) * 2 + layer,
                ).start()
                return carry

            lax.fori_loop(jnp.where(core == layer, 1, 0), 16, one, 0)

        spread(0)
        spread(1)
    send(0, 1)
    if not with_weights:
        lax.fori_loop(1, groups - 1, step, 0)
    else:
        lax.fori_loop(1, FIRST_GROUPS, step, 0)
        arrived = full_ref.at[0, :, :, 0]
        pltpu.make_async_copy(arrived, arrived, plane_recv).wait()

        def far(layer):
            copies = []
            for k in (1, 3, 2):
                if layer == 0:
                    slab = full_ref.at[0, :, :, z]
                    to = lax.rem(me + 32 * k, count)
                else:
                    slab = full_ref.at[1, :, :, :, y]
                    to = z * 32 + lax.rem(y + k, 4) * 8 + pair
                copies.append(remote(slab, slab, far_send.at[k], far_recv.at[k], to))
            return copies

        for layer in range(2):
            @pl.when(core == layer)
            def _():
                for copy in far(layer):
                    copy.start()

        lax.fori_loop(FIRST_GROUPS, groups - 1, step, 0)
    send(groups - 1, 0)
    if with_weights:
        for layer in range(2):
            @pl.when(core == layer)
            def _():
                for copy in far(layer):
                    copy.wait()
        across = remote(
            full_ref.at[core], full_ref.at[core], core_send, core_recv, me + 1 - 2 * core
        )
        across.start()
        across.wait()
        gone = full_ref.at[0, :, :, 0:3, 0, 0:5]
        pltpu.make_async_copy(gone, gone, plane_send.at[0]).wait()
        gone = full_ref.at[0, :, :, 0:2, 0]
        pltpu.make_async_copy(gone, gone, plane_send.at[1]).wait()
    some = pl.ds(0, count - 1)
    pltpu.make_async_copy(in_ref.at[some], in_ref.at[some], recv_sem).wait()
    pltpu.make_async_copy(out_ref.at[some], out_ref.at[some], send_sem).wait()


def exchange(turned, rows, weights=()):
    slots, count = turned.shape
    block = (count, slots, rows.shape[1])
    out_shape = [jax.ShapeDtypeStruct(block, rows.dtype)]
    scratch = [pltpu.VMEM(block, rows.dtype), pltpu.VMEM((count, slots), turned.dtype)]
    sems = [pltpu.SemaphoreType.DMA] * 2
    if weights:
        matrices = weights[0].shape[0] + 1
        halves = rows.shape[1] // LANES
        out_shape.append(
            jax.ShapeDtypeStruct((2, matrices, halves, 4, 4, 8, 2, LANES), rows.dtype)
        )
        scratch.append(pltpu.VMEM((2, matrices, halves, 2, LANES), rows.dtype))
        sems += [pltpu.SemaphoreType.DMA((2,)), pltpu.SemaphoreType.DMA]
        sems += [pltpu.SemaphoreType.DMA((4,))] * 2 + [pltpu.SemaphoreType.DMA] * 2
    return pl.pallas_call(
        functools.partial(exchange_body, count, bool(weights)),
        out_shape=out_shape,
        in_specs=[VMEM] * (2 + len(weights)),
        out_specs=[ANY] * len(out_shape),
        scratch_shapes=scratch + sems,
        compiler_params=pltpu.CompilerParams(
            collective_id=0 if weights else 1,
            has_side_effects=True,
            vmem_limit_bytes=LIMIT,
        ),
        name="exchange_weights" if weights else "exchange",
    )(turned, rows, *weights)


def layer_body(
    relu,
    layer,
    count_ref,
    source_ref,
    target_ref,
    relation_ref,
    own_hbm,
    recv_hbm,
    weight_hbm,
    bias_ref,
    out_ref,
    table,
    pooled,
    counts,
    stage_a,
    stage_b,
    own_ref,
    recv_ref,
    weight_ref,
    doubled,
    window_row,
    window_ref,
    ids_0,
    ids_1,
    ids_2,
    ids_3,
    own_sem,
    recv_sem,
    weight_sem,
    window_sem,
    ids_sem,
):
    nodes, width = own_ref.shape
    relations = weight_ref.shape[0] - 1
    blocks, block_width = target_ref.shape
    slots = WIN * relations
    chunk = 256
    pieces = recv_sem.shape[0]
    piece = recv_ref.shape[0] // pieces

    own_copy = pltpu.make_async_copy(own_hbm, own_ref, own_sem)
    own_copy.start()
    recv_copies = []
    for p in range(pieces):
        rows = pl.ds(p * piece, piece)
        copy = pltpu.make_async_copy(recv_hbm.at[rows], recv_ref.at[rows], recv_sem.at[p])
        copy.start()
        recv_copies.append(copy)
    weight_copy = pltpu.make_async_copy(weight_hbm.at[layer], weight_ref, weight_sem)
    weight_copy.start()

    chunks, rows_per_chunk = doubled.shape[:2]
    for c in range(chunks):
        doubled[c] = source_ref[pl.ds(c * rows_per_chunk, rows_per_chunk), :] * 2
    first = target_ref[...].T
    window_row[...] = lax.shift_right_logical(first[:8, :], 4)

    def clear(i, carry):
        at = pl.multiple_of(i * slots, slots)
        pooled[pl.ds(at, slots), :] = jnp.zeros((slots, width), jnp.float32)
        counts[pl.ds(at, slots), :] = jnp.zeros((slots, LANES), jnp.float32)
        return carry

    lax.fori_loop(0, nodes // WIN, clear, 0)
    stage_b[...] = jnp.zeros_like(stage_b)

    ids = (ids_0, ids_1, ids_2, ids_3)

    def fetch(chunk, j):
        return pltpu.make_async_copy(
            doubled.at[jnp.minimum(chunk, chunks - 1)], ids[j], ids_sem.at[j]
        )

    window_copy = pltpu.make_async_copy(window_row, window_ref, window_sem)
    window_copy.start()
    for j in range(len(ids)):
        fetch(j, j).start()

    def fill(src_ref, first, last, base):
        def step(i, carry):
            rows = src_ref[pl.ds(pl.multiple_of(i * chunk, chunk), chunk), :].astype(jnp.float32)
            at = pl.multiple_of(base + i * 2 * chunk, 2 * chunk)
            table[pl.ds(at, chunk, stride=2), :] = rows[:, :LANES]
            table[pl.ds(at + 1, chunk, stride=2), :] = rows[:, LANES:]
            return carry

        lax.fori_loop(first, last, step, 0)

    own_copy.wait()
    fill(own_ref, 0, nodes // chunk, 0)
    for p in range(pieces):
        recv_copies[p].wait()
        fill(recv_ref, p * piece // chunk, (p + 1) * piece // chunk, 2 * nodes)

    used = count_ref[0]

    def gather(id_ref, first_row, stage):
        for h in range(2):
            for e in range(block_width):
                at = pl.multiple_of(id_ref[first_row + h, e], 2)
                stage[pl.ds(2 * (h * block_width + e), 2), :] = table[pl.ds(at, 2), :]

    def pool(pair, stage):
        known = jnp.maximum(pair, 0)
        slot = []
        for h in range(2):
            row = pl.ds(2 * known + h, 1)
            in_use = jnp.logical_and(pair >= 0, 2 * pair + h < used)
            shift = jnp.where(in_use, h * slots, 2 * slots)
            slot.append(
                relation_ref[row, :] * WIN + lax.bitwise_and(target_ref[row, :], WIN - 1) + shift
            )
        both = jnp.concatenate(slot, axis=1)
        hot = (
            both == lax.broadcasted_iota(jnp.int32, (2 * slots, 2 * block_width), 0)
        ).astype(jnp.float32).astype(jnp.bfloat16)
        edges = 2 * block_width
        data = jnp.concatenate(
            [
                stage[pl.ds(0, edges, stride=2), :].astype(jnp.bfloat16),
                stage[pl.ds(1, edges, stride=2), :].astype(jnp.bfloat16),
                jnp.ones((edges, LANES), jnp.bfloat16),
            ],
            axis=1,
        )
        got = jnp.dot(hot, data, preferred_element_type=jnp.float32)
        for h in range(2):
            at = pl.multiple_of(window_ref[0, 2 * known + h] * slots, slots)
            rows = pl.ds(at, slots)
            pooled[rows, :] += got[h * slots : (h + 1) * slots, :width]
            counts[rows, :] += got[h * slots : (h + 1) * slots, width:]

    pairs_per_step = len(ids) * rows_per_chunk // 2
    stages = (stage_a, stage_b)
    window_copy.wait()

    def step(i, carry):
        for j in range(len(ids)):
            fetch(0, j).wait()
            for k in range(rows_per_chunk // 2):
                n = j * rows_per_chunk // 2 + k
                gather(ids[j], 2 * k, stages[n % 2])
                pool(i * pairs_per_step + n - 1, stages[(n + 1) % 2])
            fetch((i + 1) * len(ids) + j, j).start()
        return carry

    steps = (used + 2 * pairs_per_step - 1) // (2 * pairs_per_step)
    lax.fori_loop(0, steps, step, 0)
    pool(steps * pairs_per_step - 1, stage_b)
    for j in range(len(ids)):
        fetch(0, j).wait()

    weight_copy.wait()
    part = 256
    windows = part // WIN

    def finish(i, carry):
        at = pl.multiple_of(i * part, part)
        own = own_ref[pl.ds(at, part), :]

        def weight(r):
            return jnp.concatenate([weight_ref[r, 0], weight_ref[r, 1]], axis=1)

        total = bias_ref[...] + jnp.dot(
            own, weight(relations), preferred_element_type=jnp.float32
        )
        base = pl.multiple_of(i * windows * slots, windows * slots)
        sums = pooled[pl.ds(base, windows * slots), :].reshape(windows, relations, WIN, width)
        tally = counts[pl.ds(base, windows * slots), :].reshape(windows, relations, WIN, LANES)
        for r in range(relations):
            inverse = 1.0 / jnp.maximum(tally[:, r].reshape(part, LANES), 1.0)
            sums_r = sums[:, r].reshape(part, width)
            mean = jnp.concatenate(
                [sums_r[:, :LANES] * inverse, sums_r[:, LANES:] * inverse], axis=1
            ).astype(jnp.bfloat16)
            total = total + jnp.dot(mean, weight(r), preferred_element_type=jnp.float32)
        if relu:
            total = jnp.maximum(total, 0.0)
        out_ref[pl.ds(at, part), :] = total.astype(jnp.bfloat16)
        return carry

    lax.fori_loop(0, nodes // part, finish, 0)


def relational_layer(
    layer, rows, received, count, sources, targets, relation_ids, weights, bias
):
    nodes, width = rows.shape
    relations = weights.shape[1] - 1
    table_rows = 2 * (nodes + received.shape[0])
    pieces = 4
    return pl.pallas_call(
        functools.partial(layer_body, layer == 0, layer),
        out_shape=jax.ShapeDtypeStruct((nodes, width), jnp.bfloat16),
        in_specs=[SMEM, VMEM, VMEM, VMEM, ANY, ANY, ANY, VMEM],
        out_specs=VMEM,
        scratch_shapes=[
            pltpu.VMEM((table_rows, LANES), jnp.float32),
            pltpu.VMEM((nodes * relations, width), jnp.float32),
            pltpu.VMEM((nodes * relations, LANES), jnp.float32),
            pltpu.VMEM((4 * LANES, LANES), jnp.float32),
            pltpu.VMEM((4 * LANES, LANES), jnp.float32),
            pltpu.VMEM(rows.shape, rows.dtype),
            pltpu.VMEM(received.shape, received.dtype),
            pltpu.VMEM(weights.shape[1:], weights.dtype),
            pltpu.VMEM((sources.shape[0] // 4, 4, LANES), sources.dtype),
            pltpu.VMEM((8, LANES), sources.dtype),
            pltpu.SMEM((8, LANES), sources.dtype),
            pltpu.SMEM((4, LANES), sources.dtype),
            pltpu.SMEM((4, LANES), sources.dtype),
            pltpu.SMEM((4, LANES), sources.dtype),
            pltpu.SMEM((4, LANES), sources.dtype),
            pltpu.SemaphoreType.DMA,
            pltpu.SemaphoreType.DMA((pieces,)),
            pltpu.SemaphoreType.DMA,
            pltpu.SemaphoreType.DMA,
            pltpu.SemaphoreType.DMA((4,)),
        ],
        compiler_params=pltpu.CompilerParams(vmem_limit_bytes=LIMIT),
        name="relational_layer",
    )(
        count, sources, targets, relation_ids, rows, received, weights,
        bias.reshape(1, width),
    )


def shards(
    features,
    edge_source,
    edge_relation,
    edge_target,
    block_count,
    send_list,
    bases_first,
    self_first,
    coef_first,
    bias_first,
    bases_second,
    self_second,
    coef_second,
    bias_second,
):
    edges = (block_count, edge_source[0], edge_target[0], edge_relation[0])
    turned = jnp.swapaxes(send_list[0], 0, 1)
    width = features.shape[1]
    received, full = exchange(
        turned,
        features,
        (coef_first, bases_first, self_first, coef_second, bases_second, self_second),
    )
    full = full.reshape(full.shape[:3] + (width, LANES))
    hidden = relational_layer(
        0, features, received.reshape(-1, width), *edges, full, bias_first
    )
    (received,) = exchange(turned, hidden)
    return relational_layer(
        1, hidden, received.reshape(-1, width), *edges, full, bias_second
    )


def solution(mesh):
    placed = (
        P("dom", None),
        P("dom", None, None),
        P("dom", None, None),
        P("dom", None, None),
        P("dom"),
        P("dom", None, None),
        P(None, "dom", None),
        P("dom", None),
        P(),
        P(),
        P(None, "dom", None),
        P("dom", None),
        P(),
        P(),
    )
    return jax.shard_map(
        shards, mesh=mesh, in_specs=placed, out_specs=P("dom", None), check_vma=False
    )
```

```python
import functools

import jax
import jax.numpy as jnp
from jax import lax
from jax.experimental import pallas as pl
from jax.experimental.pallas import tpu as pltpu
from jax.sharding import PartitionSpec as P

WIN = 16
LANES = 128
VMEM = pl.BlockSpec(memory_space=pltpu.VMEM)
SMEM = pl.BlockSpec(memory_space=pltpu.SMEM)
LIMIT = 60 * 1024 * 1024


def mix_weights(layer, coef_ref, bases_ref, self_ref, part_ref):
    relations = coef_ref.shape[0]
    rows = []
    for i in range(2):
        bases = bases_ref[:, i, :].astype(jnp.float32)
        rows.append(
            jnp.dot(
                coef_ref[...],
                bases,
                precision=lax.Precision.HIGHEST,
                preferred_element_type=jnp.float32,
            )
        )
    for h in range(2):
        lanes = slice(h * LANES, (h + 1) * LANES)
        for r in range(relations):
            both = jnp.concatenate([row[r : r + 1, lanes] for row in rows], axis=0)
            part_ref[layer, r, h] = both.astype(jnp.bfloat16)
        part_ref[layer, relations, h] = self_ref[:, lanes]


MESH = pl.DeviceIdType.MESH
ANY = pl.BlockSpec(memory_space=pl.ANY)
GROUP = 8
FIRST_GROUPS = 6
CHUNK_BLOCKS = 8


def rows_of_group(group, send_ref, rows_ref, out_ref):
    slots = send_ref.shape[1]
    nodes, width = rows_ref.shape
    ids = send_ref[pl.ds(pl.multiple_of(group * GROUP, GROUP), GROUP), :]
    hot = (
        (ids[:, :, None] == lax.broadcasted_iota(jnp.int32, (GROUP, slots, nodes), 2))
        .astype(jnp.float32)
        .astype(jnp.bfloat16)
        .reshape(GROUP * slots, nodes)
    )
    got = jnp.dot(hot, rows_ref[...], preferred_element_type=jnp.float32)
    out_ref[pl.ds(group * GROUP, GROUP)] = got.astype(jnp.bfloat16).reshape(GROUP, slots, width)


def remote(src, dst, send_sem, recv_sem, to):
    return pltpu.make_async_remote_copy(
        src_ref=src,
        dst_ref=dst,
        send_sem=send_sem,
        recv_sem=recv_sem,
        device_id=(to,),
        device_id_type=MESH,
    )


def tally_slots(target_ref, relation_ref, tally_ref):
    blocks, block_width = target_ref.shape
    slots = tally_ref.shape[1]
    lane = lax.broadcasted_iota(jnp.int32, (8, 2 * block_width), 1) // block_width
    row = lax.broadcasted_iota(jnp.int32, (8, 2 * block_width), 0)
    slot_ids = lax.broadcasted_iota(jnp.int32, (slots, 2 * block_width), 0)

    def tally(g, carry):
        at = pl.ds(pl.multiple_of(8 * g, 8), 8)
        slot = relation_ref[at, :] * WIN + lax.bitwise_and(target_ref[at, :], WIN - 1)
        total = jnp.zeros((8, slots), jnp.float32)
        for p in range(4):
            both = jnp.concatenate([slot[2 * p : 2 * p + 1], slot[2 * p + 1 : 2 * p + 2]], axis=1)
            hot = (both == slot_ids).astype(jnp.float32).astype(jnp.bfloat16)
            pick = (row == lane + 2 * p).astype(jnp.float32).astype(jnp.bfloat16)
            total = total + lax.dot_general(
                pick, hot, (((1,), (1,)), ((), ())), preferred_element_type=jnp.float32
            )
        tally_ref[at, :] = total
        return carry

    lax.fori_loop(0, blocks // 8, tally, 0)


def invert_degrees(count_ref, target_ref, tally_ref, windows):
    blocks = target_ref.shape[0]
    window = lax.shift_right_logical(target_ref[...].T[:1, :], 4)
    in_use = lax.broadcasted_iota(jnp.int32, (windows, blocks), 1) < count_ref[0]
    same = window == lax.broadcasted_iota(jnp.int32, (windows, blocks), 0)
    held = jnp.logical_and(same, in_use).astype(jnp.float32).astype(jnp.bfloat16)
    degree = jnp.dot(
        held, tally_ref[...].astype(jnp.bfloat16), preferred_element_type=jnp.float32
    )
    tally_ref[:windows, :] = 1.0 / jnp.maximum(degree, 1.0)


def spread_windows(first, last, tally_ref, inverse_ref):
    slots = tally_ref.shape[1]

    def spread(w, carry):
        row = jnp.broadcast_to(tally_ref[pl.ds(w, 1), :], (slots, slots))
        inverse_ref[pl.ds(pl.multiple_of(w * slots, slots), slots), :] = row.T
        return carry

    lax.fori_loop(first, last, spread, 0)


def exchange_body(count, with_weights, *refs):
    if with_weights:
        (turned_ref, rows_ref, coef_a, bases_a, self_a, coef_b, bases_b, self_b,
         count_ref, target_ref, relation_ref,
         in_ref, full_ref, inverse_out, out_ref, send_ref, part_ref, tally_ref, inverse_ref,
         send_sem, recv_sem, plane_send, plane_recv, far_send, far_recv, core_send, core_recv,
         inverse_sem) = refs
    else:
        turned_ref, rows_ref, in_ref, out_ref, send_ref, send_sem, recv_sem = refs
    me = lax.axis_index("dom")
    groups = count // GROUP
    barrier = pltpu.get_barrier_semaphore()

    for k in range(1, count):
        pl.semaphore_signal(
            barrier, inc=1, device_id=(lax.rem(me + k, count),), device_id_type=MESH
        )

    def group_at(t):
        return lax.rem(me // GROUP + 5 * t, groups)

    def compute(t):
        rows_of_group(group_at(t), send_ref, rows_ref, out_ref)

    def send(t, first):
        for i in range(first, GROUP):
            to = group_at(t) * GROUP + lax.rem(me + i, GROUP)
            remote(out_ref.at[to], in_ref.at[me], send_sem, recv_sem, to).start()

    def step(t, carry):
        compute(t + 1)
        send(t, 0)
        return carry

    send_ref[...] = turned_ref[...].T
    if with_weights:
        mix_weights(0, coef_a, bases_a, self_a, part_ref)
        mix_weights(1, coef_b, bases_b, self_b, part_ref)
    compute(0)
    compute(1)
    pl.semaphore_wait(barrier, count - 1)
    if with_weights:
        core = lax.rem(me, 2)
        x = lax.rem(me // 2, 4)
        y = lax.rem(me // 8, 4)
        z = me // 32
        pair = lax.rem(me, 8)
        mine = pltpu.make_async_copy(
            part_ref.at[core], full_ref.at[core, :, :, z, y, pair], plane_recv
        )
        mine.start()

        def spread(layer):
            def one(k, carry):
                column = lax.rem(x + k, 4)
                if layer == 0:
                    line = (z * 4 + lax.rem(y + k // 4, 4)) * 4
                else:
                    line = (lax.rem(z + k // 4, 4) * 4 + y) * 4
                remote(
                    part_ref.at[layer],
                    full_ref.at[layer, :, :, z, y, pair],
                    plane_send.at[jnp.where(core == layer, 0, 1)],
                    plane_recv,
                    (line + column) * 2 + layer,
                ).start()
                return carry

            lax.fori_loop(jnp.where(core == layer, 1, 0), 16, one, 0)

        spread(0)
        spread(1)
    send(0, 1)
    if not with_weights:
        lax.fori_loop(1, groups - 1, step, 0)
    else:
        lax.fori_loop(1, FIRST_GROUPS, step, 0)
        arrived = full_ref.at[0, :, :, 0]
        pltpu.make_async_copy(arrived, arrived, plane_recv).wait()

        def slab_of(layer, back):
            if layer == 0:
                return full_ref.at[0, :, :, lax.rem(z + 4 - back, 4)]
            return full_ref.at[1, :, :, :, lax.rem(y + 4 - back, 4)]

        def far(layer, k):
            slab = slab_of(layer, 0)
            if layer == 0:
                to = lax.rem(me + 32 * k, count)
            else:
                to = z * 32 + lax.rem(y + k, 4) * 8 + pair
            return remote(slab, slab, far_send.at[k], far_recv.at[k], to)

        def across(layer, k):
            slab = slab_of(layer, k)
            return remote(slab, slab, core_send.at[k], core_recv.at[k], me + 1 - 2 * core)

        for layer in range(2):
            @pl.when(core == layer)
            def _():
                for k in (1, 3, 2):
                    far(layer, k).start()
                across(layer, 0).start()

        lax.fori_loop(FIRST_GROUPS, groups - 1, step, 0)
    send(groups - 1, 0)
    if with_weights:
        tally_slots(target_ref, relation_ref, tally_ref)
        slots = tally_ref.shape[1]
        windows = inverse_ref.shape[0] // slots
        quarter = windows // 4
        invert_degrees(count_ref, target_ref, tally_ref, windows)

        def put(q):
            rows = pl.ds(q * quarter * slots, quarter * slots)
            return pltpu.make_async_copy(
                inverse_ref.at[rows], inverse_out.at[rows], inverse_sem.at[q]
            )

        for q in range(4):
            spread_windows(q * quarter, (q + 1) * quarter, tally_ref, inverse_ref)
            if q > 0:
                put(q - 1).start()
        for layer in range(2):
            @pl.when(core == layer)
            def _():
                for k in (1, 3, 2):
                    far(layer, k).wait_recv()
                    across(layer, k).start()
        for layer in range(2):
            @pl.when(core == layer)
            def _():
                for k in (1, 3, 2):
                    far(layer, k).wait_send()
                for k in (0, 1, 3, 2):
                    across(layer, k).wait()
        put(3).start()
        for q in range(4):
            put(q).wait()
        gone = full_ref.at[0, :, :, 0:3, 0, 0:5]
        pltpu.make_async_copy(gone, gone, plane_send.at[0]).wait()
        gone = full_ref.at[0, :, :, 0:2, 0]
        pltpu.make_async_copy(gone, gone, plane_send.at[1]).wait()
    some = pl.ds(0, count - 1)
    pltpu.make_async_copy(in_ref.at[some], in_ref.at[some], recv_sem).wait()
    pltpu.make_async_copy(out_ref.at[some], out_ref.at[some], send_sem).wait()


def exchange(turned, rows, weights=(), edges=()):
    slots, count = turned.shape
    block = (count, slots, rows.shape[1])
    out_shape = [jax.ShapeDtypeStruct(block, rows.dtype)]
    scratch = [pltpu.VMEM(block, rows.dtype), pltpu.VMEM((count, slots), turned.dtype)]
    sems = [pltpu.SemaphoreType.DMA] * 2
    if weights:
        matrices = weights[0].shape[0] + 1
        halves = rows.shape[1] // LANES
        out_shape.append(
            jax.ShapeDtypeStruct((2, matrices, halves, 4, 4, 8, 2, LANES), rows.dtype)
        )
        slots = (matrices - 1) * WIN
        scratch.append(pltpu.VMEM((2, matrices, halves, 2, LANES), rows.dtype))
        scratch.append(pltpu.VMEM((edges[1].shape[0], slots), jnp.float32))
        inverse = (rows.shape[0] * (matrices - 1), LANES)
        scratch.append(pltpu.VMEM(inverse, jnp.float32))
        out_shape.append(jax.ShapeDtypeStruct(inverse, jnp.float32))
        sems += [pltpu.SemaphoreType.DMA((2,)), pltpu.SemaphoreType.DMA]
        sems += [pltpu.SemaphoreType.DMA((4,))] * 5
    return pl.pallas_call(
        functools.partial(exchange_body, count, bool(weights)),
        out_shape=out_shape,
        in_specs=[VMEM] * (2 + len(weights)) + [SMEM, VMEM, VMEM][: len(edges)],
        out_specs=[ANY] * len(out_shape),
        scratch_shapes=scratch + sems,
        compiler_params=pltpu.CompilerParams(
            collective_id=0 if weights else 1,
            has_side_effects=True,
            vmem_limit_bytes=LIMIT,
        ),
        name="exchange_weights" if weights else "exchange",
    )(turned, rows, *weights, *edges)


def layer_body(
    relu,
    layer,
    count_ref,
    source_ref,
    target_ref,
    relation_ref,
    own_hbm,
    recv_hbm,
    weight_hbm,
    inverse_hbm,
    bias_ref,
    out_ref,
    table,
    pooled,
    inverse_ref,
    stage_a,
    stage_b,
    own_ref,
    recv_ref,
    weight_ref,
    doubled,
    window_row,
    window_ref,
    ids_0,
    ids_1,
    own_sem,
    recv_sem,
    weight_sem,
    inverse_sem,
    window_sem,
    ids_sem,
):
    nodes, width = own_ref.shape
    relations = weight_ref.shape[0] - 1
    blocks, block_width = target_ref.shape
    slots = WIN * relations
    chunk = 256
    pieces = recv_sem.shape[0]
    piece = recv_ref.shape[0] // pieces

    own_copy = pltpu.make_async_copy(own_hbm, own_ref, own_sem)
    own_copy.start()
    recv_copies = []
    for p in range(pieces):
        rows = pl.ds(p * piece, piece)
        copy = pltpu.make_async_copy(recv_hbm.at[rows], recv_ref.at[rows], recv_sem.at[p])
        copy.start()
        recv_copies.append(copy)
    weight_copy = pltpu.make_async_copy(weight_hbm.at[layer], weight_ref, weight_sem)
    weight_copy.start()
    inverse_copy = pltpu.make_async_copy(inverse_hbm, inverse_ref, inverse_sem)
    inverse_copy.start()

    rows_per_chunk = ids_0.shape[0]
    chunks = blocks // rows_per_chunk
    doubled[...] = source_ref[...] * 2
    first = target_ref[...].T
    window_row[...] = lax.shift_right_logical(first[:8, :], 4)

    def clear(i, carry):
        at = pl.multiple_of(i * slots, slots)
        pooled[pl.ds(at, slots), :] = jnp.zeros((slots, width), jnp.float32)
        return carry

    lax.fori_loop(0, nodes // WIN, clear, 0)
    stage_b[...] = jnp.zeros_like(stage_b)

    ids = (ids_0, ids_1)

    def fetch(chunk, j):
        first_row = pl.multiple_of(
            jnp.minimum(chunk, chunks - 1) * rows_per_chunk, rows_per_chunk
        )
        return pltpu.make_async_copy(
            doubled.at[pl.ds(first_row, rows_per_chunk)], ids[j], ids_sem.at[j]
        )

    window_copy = pltpu.make_async_copy(window_row, window_ref, window_sem)
    window_copy.start()
    for j in range(len(ids)):
        fetch(j, j).start()

    def fill(src_ref, first, last, base):
        def step(i, carry):
            rows = src_ref[pl.ds(pl.multiple_of(i * chunk, chunk), chunk), :].astype(jnp.float32)
            at = pl.multiple_of(base + i * 2 * chunk, 2 * chunk)
            table[pl.ds(at, chunk, stride=2), :] = rows[:, :LANES]
            table[pl.ds(at + 1, chunk, stride=2), :] = rows[:, LANES:]
            return carry

        lax.fori_loop(first, last, step, 0)

    own_copy.wait()
    fill(own_ref, 0, nodes // chunk, 0)
    for p in range(pieces):
        recv_copies[p].wait()
        fill(recv_ref, p * piece // chunk, (p + 1) * piece // chunk, 2 * nodes)

    used = count_ref[0]

    def gather(id_ref, first_row, stage):
        for h in range(2):
            for e in range(block_width):
                at = pl.multiple_of(id_ref[first_row + h, e], 2)
                stage[pl.ds(2 * (h * block_width + e), 2), :] = table[pl.ds(at, 2), :]

    def pool(pair, stage):
        known = jnp.maximum(pair, 0)
        slot = []
        for h in range(2):
            row = pl.ds(2 * known + h, 1)
            in_use = jnp.logical_and(pair >= 0, 2 * pair + h < used)
            shift = jnp.where(in_use, h * slots, 2 * slots)
            slot.append(
                relation_ref[row, :] * WIN + lax.bitwise_and(target_ref[row, :], WIN - 1) + shift
            )
        both = jnp.concatenate(slot, axis=1)
        hot = (
            both == lax.broadcasted_iota(jnp.int32, (2 * slots, 2 * block_width), 0)
        ).astype(jnp.float32).astype(jnp.bfloat16)
        edges = 2 * block_width
        data = jnp.concatenate(
            [
                stage[pl.ds(0, edges, stride=2), :].astype(jnp.bfloat16),
                stage[pl.ds(1, edges, stride=2), :].astype(jnp.bfloat16),
            ],
            axis=1,
        )
        got = jnp.dot(hot, data, preferred_element_type=jnp.float32)
        for h in range(2):
            at = pl.multiple_of(window_ref[0, 2 * known + h] * slots, slots)
            rows = pl.ds(at, slots)
            pooled[rows, :] += got[h * slots : (h + 1) * slots]

    pairs_per_step = len(ids) * rows_per_chunk // 2
    stages = (stage_a, stage_b)
    window_copy.wait()

    def step(i, carry):
        for j in range(len(ids)):
            fetch(0, j).wait()
            for k in range(rows_per_chunk // 2):
                n = j * rows_per_chunk // 2 + k
                pool(i * pairs_per_step + n - 1, stages[(n + 1) % 2])
                gather(ids[j], 2 * k, stages[n % 2])
            fetch((i + 1) * len(ids) + j, j).start()
        return carry

    steps = (used + 2 * pairs_per_step - 1) // (2 * pairs_per_step)
    lax.fori_loop(0, steps, step, 0)
    pool(steps * pairs_per_step - 1, stage_b)
    for j in range(len(ids)):
        fetch(0, j).wait()

    weight_copy.wait()
    inverse_copy.wait()
    part = 256
    windows = part // WIN

    def finish(i, carry):
        at = pl.multiple_of(i * part, part)
        own = own_ref[pl.ds(at, part), :]

        def weight(r):
            return jnp.concatenate([weight_ref[r, 0], weight_ref[r, 1]], axis=1)

        total = bias_ref[...] + jnp.dot(
            own, weight(relations), preferred_element_type=jnp.float32
        )
        base = pl.multiple_of(i * windows * slots, windows * slots)
        sums = pooled[pl.ds(base, windows * slots), :].reshape(windows, relations, WIN, width)
        scale = inverse_ref[pl.ds(base, windows * slots), :].reshape(
            windows, relations, WIN, LANES
        )
        for r in range(relations):
            inverse = scale[:, r].reshape(part, LANES)
            sums_r = sums[:, r].reshape(part, width)
            mean = jnp.concatenate(
                [sums_r[:, :LANES] * inverse, sums_r[:, LANES:] * inverse], axis=1
            ).astype(jnp.bfloat16)
            total = total + jnp.dot(mean, weight(r), preferred_element_type=jnp.float32)
        if relu:
            total = jnp.maximum(total, 0.0)
        out_ref[pl.ds(at, part), :] = total.astype(jnp.bfloat16)
        return carry

    lax.fori_loop(0, nodes // part, finish, 0)


def relational_layer(
    layer, rows, received, count, sources, targets, relation_ids, weights, inverse, bias
):
    nodes, width = rows.shape
    relations = weights.shape[1] - 1
    table_rows = 2 * (nodes + received.shape[0])
    pieces = 4
    return pl.pallas_call(
        functools.partial(layer_body, layer == 0, layer),
        out_shape=jax.ShapeDtypeStruct((nodes, width), jnp.bfloat16),
        in_specs=[SMEM, VMEM, VMEM, VMEM, ANY, ANY, ANY, ANY, VMEM],
        out_specs=VMEM,
        scratch_shapes=[
            pltpu.VMEM((table_rows, LANES), jnp.float32),
            pltpu.VMEM((nodes * relations, width), jnp.float32),
            pltpu.VMEM((nodes * relations, LANES), jnp.float32),
            pltpu.VMEM((4 * LANES, LANES), jnp.float32),
            pltpu.VMEM((4 * LANES, LANES), jnp.float32),
            pltpu.VMEM(rows.shape, rows.dtype),
            pltpu.VMEM(received.shape, received.dtype),
            pltpu.VMEM(weights.shape[1:], weights.dtype),
            pltpu.VMEM(sources.shape, sources.dtype),
            pltpu.VMEM((8, LANES), sources.dtype),
            pltpu.SMEM((8, LANES), sources.dtype),
            pltpu.SMEM((CHUNK_BLOCKS, LANES), sources.dtype),
            pltpu.SMEM((CHUNK_BLOCKS, LANES), sources.dtype),
            pltpu.SemaphoreType.DMA,
            pltpu.SemaphoreType.DMA((pieces,)),
            pltpu.SemaphoreType.DMA,
            pltpu.SemaphoreType.DMA,
            pltpu.SemaphoreType.DMA,
            pltpu.SemaphoreType.DMA((2,)),
        ],
        compiler_params=pltpu.CompilerParams(
            vmem_limit_bytes=LIMIT,
        ),
        name="relational_layer",
    )(
        count, sources, targets, relation_ids, rows, received, weights, inverse,
        bias.reshape(1, width),
    )


def shards(
    features,
    edge_source,
    edge_relation,
    edge_target,
    block_count,
    send_list,
    bases_first,
    self_first,
    coef_first,
    bias_first,
    bases_second,
    self_second,
    coef_second,
    bias_second,
):
    edges = (block_count, edge_source[0], edge_target[0], edge_relation[0])
    turned = jnp.swapaxes(send_list[0], 0, 1)
    width = features.shape[1]
    received, full, inverse = exchange(
        turned,
        features,
        (coef_first, bases_first, self_first, coef_second, bases_second, self_second),
        (block_count, edge_target[0], edge_relation[0]),
    )
    full = full.reshape(full.shape[:3] + (width, LANES))
    hidden = relational_layer(
        0, features, received.reshape(-1, width), *edges, full, inverse, bias_first
    )
    (received,) = exchange(turned, hidden)
    return relational_layer(
        1, hidden, received.reshape(-1, width), *edges, full, inverse, bias_second
    )


def solution(mesh):
    placed = (
        P("dom", None),
        P("dom", None, None),
        P("dom", None, None),
        P("dom", None, None),
        P("dom"),
        P("dom", None, None),
        P(None, "dom", None),
        P("dom", None),
        P(),
        P(),
        P(None, "dom", None),
        P("dom", None),
        P(),
        P(),
    )
    return jax.shard_map(
        shards, mesh=mesh, in_specs=placed, out_specs=P("dom", None), check_vma=False
    )
```

```python
import functools

import jax
import jax.numpy as jnp
from jax import lax
from jax.experimental import pallas as pl
from jax.experimental.pallas import tpu as pltpu
from jax.sharding import PartitionSpec as P

WIN = 16
LANES = 128
VMEM = pl.BlockSpec(memory_space=pltpu.VMEM)
SMEM = pl.BlockSpec(memory_space=pltpu.SMEM)
LIMIT = 60 * 1024 * 1024


def mix_weights(layer, coef_ref, bases_ref, self_ref, part_ref):
    relations = coef_ref.shape[0]
    rows = []
    for i in range(2):
        bases = bases_ref[:, i, :].astype(jnp.float32)
        rows.append(
            jnp.dot(
                coef_ref[...],
                bases,
                precision=lax.Precision.HIGHEST,
                preferred_element_type=jnp.float32,
            )
        )
    for h in range(2):
        lanes = slice(h * LANES, (h + 1) * LANES)
        for r in range(relations):
            both = jnp.concatenate([row[r : r + 1, lanes] for row in rows], axis=0)
            part_ref[layer, r, h] = both.astype(jnp.bfloat16)
        part_ref[layer, relations, h] = self_ref[:, lanes]


MESH = pl.DeviceIdType.MESH
ANY = pl.BlockSpec(memory_space=pl.ANY)
GROUP = 8
FIRST_GROUPS = 6
CHUNK_BLOCKS = 16


def rows_of_group(group, send_ref, rows_ref, out_ref):
    slots = send_ref.shape[1]
    nodes, width = rows_ref.shape
    ids = send_ref[pl.ds(pl.multiple_of(group * GROUP, GROUP), GROUP), :]
    hot = (
        (ids[:, :, None] == lax.broadcasted_iota(jnp.int32, (GROUP, slots, nodes), 2))
        .astype(jnp.float32)
        .astype(jnp.bfloat16)
        .reshape(GROUP * slots, nodes)
    )
    got = jnp.dot(hot, rows_ref[...], preferred_element_type=jnp.float32)
    out_ref[pl.ds(group * GROUP, GROUP)] = got.astype(jnp.bfloat16).reshape(GROUP, slots, width)


def remote(src, dst, send_sem, recv_sem, to):
    return pltpu.make_async_remote_copy(
        src_ref=src,
        dst_ref=dst,
        send_sem=send_sem,
        recv_sem=recv_sem,
        device_id=(to,),
        device_id_type=MESH,
    )


def tally_slots(target_ref, relation_ref, tally_ref):
    blocks, block_width = target_ref.shape
    slots = tally_ref.shape[1]
    lane = lax.broadcasted_iota(jnp.int32, (8, 2 * block_width), 1) // block_width
    row = lax.broadcasted_iota(jnp.int32, (8, 2 * block_width), 0)
    slot_ids = lax.broadcasted_iota(jnp.int32, (slots, 2 * block_width), 0)

    def tally(g, carry):
        at = pl.ds(pl.multiple_of(8 * g, 8), 8)
        slot = relation_ref[at, :] * WIN + lax.bitwise_and(target_ref[at, :], WIN - 1)
        total = jnp.zeros((8, slots), jnp.float32)
        for p in range(4):
            both = jnp.concatenate([slot[2 * p : 2 * p + 1], slot[2 * p + 1 : 2 * p + 2]], axis=1)
            hot = (both == slot_ids).astype(jnp.float32).astype(jnp.bfloat16)
            pick = (row == lane + 2 * p).astype(jnp.float32).astype(jnp.bfloat16)
            total = total + lax.dot_general(
                pick, hot, (((1,), (1,)), ((), ())), preferred_element_type=jnp.float32
            )
        tally_ref[at, :] = total
        return carry

    lax.fori_loop(0, blocks // 8, tally, 0)


def invert_degrees(count_ref, target_ref, tally_ref, windows):
    blocks = target_ref.shape[0]
    window = lax.shift_right_logical(target_ref[...].T[:1, :], 4)
    in_use = lax.broadcasted_iota(jnp.int32, (windows, blocks), 1) < count_ref[0]
    same = window == lax.broadcasted_iota(jnp.int32, (windows, blocks), 0)
    held = jnp.logical_and(same, in_use).astype(jnp.float32).astype(jnp.bfloat16)
    degree = jnp.dot(
        held, tally_ref[...].astype(jnp.bfloat16), preferred_element_type=jnp.float32
    )
    tally_ref[:windows, :] = 1.0 / jnp.maximum(degree, 1.0)


def spread_windows(first, last, tally_ref, inverse_ref):
    slots = tally_ref.shape[1]

    def spread(w, carry):
        row = jnp.broadcast_to(tally_ref[pl.ds(w, 1), :], (slots, slots))
        inverse_ref[pl.ds(pl.multiple_of(w * slots, slots), slots), :] = row.T
        return carry

    lax.fori_loop(first, last, spread, 0)


def exchange_body(count, with_weights, *refs):
    if with_weights:
        inputs, count_ref, refs = refs[:10], refs[10], refs[11:]
        (in_ref, full_ref, inverse_out, out_ref, send_ref, part_ref, tally_ref, inverse_ref,
         send_sem, recv_sem, plane_send, plane_recv, far_send, far_recv, core_send, core_recv,
         inverse_sem), refs = refs[:17], refs[17:]
        (turned_ref, rows_ref, coef_a, bases_a, self_a, coef_b, bases_b, self_b,
         target_ref, relation_ref) = refs[:10]
    else:
        inputs, refs = refs[:2], refs[2:]
        (in_ref, out_ref, send_ref, send_sem, recv_sem), refs = refs[:5], refs[5:]
        turned_ref, rows_ref = refs[:2]
    loads = [
        pltpu.make_async_copy(src, dst, refs[-1].at[i])
        for i, (src, dst) in enumerate(zip(inputs, refs[:-1]))
    ]
    me = lax.axis_index("dom")
    groups = count // GROUP
    barrier = pltpu.get_barrier_semaphore()

    for k in range(1, count):
        pl.semaphore_signal(
            barrier, inc=1, device_id=(lax.rem(me + k, count),), device_id_type=MESH
        )
    for load in loads:
        load.start()
    for load in loads:
        load.wait()

    def group_at(t):
        return lax.rem(me // GROUP + 5 * t, groups)

    def compute(t):
        rows_of_group(group_at(t), send_ref, rows_ref, out_ref)

    def send(t, first):
        for i in range(first, GROUP):
            to = group_at(t) * GROUP + lax.rem(me + i, GROUP)
            remote(out_ref.at[to], in_ref.at[me], send_sem, recv_sem, to).start()

    def step(t, carry):
        compute(t + 1)
        send(t, 0)
        return carry

    send_ref[...] = turned_ref[...].T
    if with_weights:
        mix_weights(0, coef_a, bases_a, self_a, part_ref)
        mix_weights(1, coef_b, bases_b, self_b, part_ref)
    compute(0)
    compute(1)
    pl.semaphore_wait(barrier, count - 1)
    if with_weights:
        core = lax.rem(me, 2)
        x = lax.rem(me // 2, 4)
        y = lax.rem(me // 8, 4)
        z = me // 32
        pair = lax.rem(me, 8)
        mine = pltpu.make_async_copy(
            part_ref.at[core], full_ref.at[core, :, :, z, y, pair], plane_recv
        )
        mine.start()

        def spread(layer):
            def one(k, carry):
                column = lax.rem(x + k, 4)
                if layer == 0:
                    line = (z * 4 + lax.rem(y + k // 4, 4)) * 4
                else:
                    line = (lax.rem(z + k // 4, 4) * 4 + y) * 4
                remote(
                    part_ref.at[layer],
                    full_ref.at[layer, :, :, z, y, pair],
                    plane_send.at[jnp.where(core == layer, 0, 1)],
                    plane_recv,
                    (line + column) * 2 + layer,
                ).start()
                return carry

            lax.fori_loop(jnp.where(core == layer, 1, 0), 16, one, 0)

        spread(0)
        spread(1)
    send(0, 1)
    if not with_weights:
        lax.fori_loop(1, groups - 1, step, 0)
    else:
        lax.fori_loop(1, FIRST_GROUPS, step, 0)
        arrived = full_ref.at[0, :, :, 0]
        pltpu.make_async_copy(arrived, arrived, plane_recv).wait()

        def slab_of(layer, back):
            if layer == 0:
                return full_ref.at[0, :, :, lax.rem(z + 4 - back, 4)]
            return full_ref.at[1, :, :, :, lax.rem(y + 4 - back, 4)]

        def far(layer, k):
            slab = slab_of(layer, 0)
            if layer == 0:
                to = lax.rem(me + 32 * k, count)
            else:
                to = z * 32 + lax.rem(y + k, 4) * 8 + pair
            return remote(slab, slab, far_send.at[k], far_recv.at[k], to)

        def across(layer, k):
            slab = slab_of(layer, k)
            return remote(slab, slab, core_send.at[k], core_recv.at[k], me + 1 - 2 * core)

        for layer in range(2):
            @pl.when(core == layer)
            def _():
                for k in (1, 3, 2):
                    far(layer, k).start()
                across(layer, 0).start()

        lax.fori_loop(FIRST_GROUPS, groups - 1, step, 0)
    send(groups - 1, 0)
    if with_weights:
        tally_slots(target_ref, relation_ref, tally_ref)
        slots = tally_ref.shape[1]
        windows = inverse_ref.shape[0] // slots
        quarter = windows // 4
        invert_degrees(count_ref, target_ref, tally_ref, windows)

        def put(q):
            rows = pl.ds(q * quarter * slots, quarter * slots)
            return pltpu.make_async_copy(
                inverse_ref.at[rows], inverse_out.at[rows], inverse_sem.at[q]
            )

        for q in range(4):
            spread_windows(q * quarter, (q + 1) * quarter, tally_ref, inverse_ref)
            if q > 0:
                put(q - 1).start()
        for layer in range(2):
            @pl.when(core == layer)
            def _():
                for k in (1, 3, 2):
                    far(layer, k).wait_recv()
                    across(layer, k).start()
        for layer in range(2):
            @pl.when(core == layer)
            def _():
                for k in (1, 3, 2):
                    far(layer, k).wait_send()
                for k in (0, 1, 3, 2):
                    across(layer, k).wait()
        put(3).start()
        for q in range(4):
            put(q).wait()
        gone = full_ref.at[0, :, :, 0:3, 0, 0:5]
        pltpu.make_async_copy(gone, gone, plane_send.at[0]).wait()
        gone = full_ref.at[0, :, :, 0:2, 0]
        pltpu.make_async_copy(gone, gone, plane_send.at[1]).wait()
    some = pl.ds(0, count - 1)
    pltpu.make_async_copy(in_ref.at[some], in_ref.at[some], recv_sem).wait()
    pltpu.make_async_copy(out_ref.at[some], out_ref.at[some], send_sem).wait()


def exchange(turned, rows, weights=(), edges=()):
    slots, count = turned.shape
    loaded = (turned, rows, *weights, *edges[1:])
    block = (count, slots, rows.shape[1])
    out_shape = [jax.ShapeDtypeStruct(block, rows.dtype)]
    scratch = [pltpu.VMEM(block, rows.dtype), pltpu.VMEM((count, slots), turned.dtype)]
    sems = [pltpu.SemaphoreType.DMA] * 2
    if weights:
        matrices = weights[0].shape[0] + 1
        halves = rows.shape[1] // LANES
        out_shape.append(
            jax.ShapeDtypeStruct((2, matrices, halves, 4, 4, 8, 2, LANES), rows.dtype)
        )
        slots = (matrices - 1) * WIN
        scratch.append(pltpu.VMEM((2, matrices, halves, 2, LANES), rows.dtype))
        scratch.append(pltpu.VMEM((edges[1].shape[0], slots), jnp.float32))
        inverse = (rows.shape[0] * (matrices - 1), LANES)
        scratch.append(pltpu.VMEM(inverse, jnp.float32))
        out_shape.append(jax.ShapeDtypeStruct(inverse, jnp.float32))
        sems += [pltpu.SemaphoreType.DMA((2,)), pltpu.SemaphoreType.DMA]
        sems += [pltpu.SemaphoreType.DMA((4,))] * 5
    return pl.pallas_call(
        functools.partial(exchange_body, count, bool(weights)),
        out_shape=out_shape,
        in_specs=[ANY] * len(loaded) + [SMEM] * len(edges[:1]),
        out_specs=[ANY] * len(out_shape),
        scratch_shapes=scratch
        + sems
        + [pltpu.VMEM(array.shape, array.dtype) for array in loaded]
        + [pltpu.SemaphoreType.DMA((len(loaded),))],
        compiler_params=pltpu.CompilerParams(
            collective_id=0 if weights else 1,
            has_side_effects=True,
            vmem_limit_bytes=LIMIT,
        ),
        name="exchange_weights" if weights else "exchange",
    )(*loaded, *edges[:1])


def layer_body(
    relu,
    layer,
    count_ref,
    source_hbm,
    target_hbm,
    relation_hbm,
    own_hbm,
    recv_hbm,
    weight_hbm,
    inverse_hbm,
    bias_hbm,
    out_ref,
    table,
    pooled,
    inverse_ref,
    stage_a,
    stage_b,
    own_ref,
    recv_ref,
    weight_ref,
    doubled,
    window_row,
    window_ref,
    ids_0,
    ids_1,
    own_sem,
    recv_sem,
    weight_sem,
    inverse_sem,
    window_sem,
    ids_sem,
    source_ref,
    target_ref,
    relation_ref,
    bias_ref,
    small_sem,
):
    nodes, width = own_ref.shape
    relations = weight_ref.shape[0] - 1
    blocks, block_width = target_ref.shape
    slots = WIN * relations
    chunk = 256
    pieces = recv_sem.shape[0]
    piece = recv_ref.shape[0] // pieces

    small = [
        pltpu.make_async_copy(src, dst, small_sem.at[i])
        for i, (src, dst) in enumerate(
            [
                (source_hbm, source_ref),
                (target_hbm, target_ref),
                (relation_hbm, relation_ref),
                (bias_hbm, bias_ref),
            ]
        )
    ]
    for copy in small:
        copy.start()
    own_copy = pltpu.make_async_copy(own_hbm, own_ref, own_sem)
    own_copy.start()
    recv_copies = []
    for p in range(pieces):
        rows = pl.ds(p * piece, piece)
        copy = pltpu.make_async_copy(recv_hbm.at[rows], recv_ref.at[rows], recv_sem.at[p])
        copy.start()
        recv_copies.append(copy)
    weight_copy = pltpu.make_async_copy(weight_hbm.at[layer], weight_ref, weight_sem)
    inverse_copy = pltpu.make_async_copy(inverse_hbm, inverse_ref, inverse_sem)
    for copy in small:
        copy.wait()

    rows_per_chunk = ids_0.shape[0]
    chunks = blocks // rows_per_chunk
    doubled[...] = source_ref[...] * 2
    first = target_ref[...].T
    window_row[...] = lax.shift_right_logical(first[:8, :], 4)

    def clear(i, carry):
        at = pl.multiple_of(i * slots, slots)
        pooled[pl.ds(at, slots), :] = jnp.zeros((slots, width), jnp.float32)
        return carry

    lax.fori_loop(0, nodes // WIN, clear, 0)
    stage_b[...] = jnp.zeros_like(stage_b)

    ids = (ids_0, ids_1)

    def fetch(chunk, j):
        first_row = pl.multiple_of(
            jnp.minimum(chunk, chunks - 1) * rows_per_chunk, rows_per_chunk
        )
        return pltpu.make_async_copy(
            doubled.at[pl.ds(first_row, rows_per_chunk)], ids[j], ids_sem.at[j]
        )

    window_copy = pltpu.make_async_copy(window_row, window_ref, window_sem)
    window_copy.start()
    for j in range(len(ids)):
        fetch(j, j).start()

    def fill(src_ref, first, last, base):
        def step(i, carry):
            rows = src_ref[pl.ds(pl.multiple_of(i * chunk, chunk), chunk), :].astype(jnp.float32)
            at = pl.multiple_of(base + i * 2 * chunk, 2 * chunk)
            table[pl.ds(at, chunk, stride=2), :] = rows[:, :LANES]
            table[pl.ds(at + 1, chunk, stride=2), :] = rows[:, LANES:]
            return carry

        lax.fori_loop(first, last, step, 0)

    own_copy.wait()
    fill(own_ref, 0, nodes // chunk, 0)
    for p in range(pieces):
        recv_copies[p].wait()
        fill(recv_ref, p * piece // chunk, (p + 1) * piece // chunk, 2 * nodes)
    weight_copy.start()
    inverse_copy.start()

    used = count_ref[0]

    def gather(id_ref, first_row, stage):
        for h in range(2):
            for e in range(block_width):
                at = pl.multiple_of(id_ref[first_row + h, e], 2)
                stage[pl.ds(2 * (h * block_width + e), 2), :] = table[pl.ds(at, 2), :]

    def pool(pair, stage):
        known = jnp.maximum(pair, 0)
        slot = []
        for h in range(2):
            row = pl.ds(2 * known + h, 1)
            in_use = jnp.logical_and(pair >= 0, 2 * pair + h < used)
            shift = jnp.where(in_use, h * slots, 2 * slots)
            slot.append(
                relation_ref[row, :] * WIN + lax.bitwise_and(target_ref[row, :], WIN - 1) + shift
            )
        both = jnp.concatenate(slot, axis=1)
        hot = (
            both == lax.broadcasted_iota(jnp.int32, (2 * slots, 2 * block_width), 0)
        ).astype(jnp.float32).astype(jnp.bfloat16)
        edges = 2 * block_width
        data = jnp.concatenate(
            [
                stage[pl.ds(0, edges, stride=2), :].astype(jnp.bfloat16),
                stage[pl.ds(1, edges, stride=2), :].astype(jnp.bfloat16),
            ],
            axis=1,
        )
        got = jnp.dot(hot, data, preferred_element_type=jnp.float32)
        for h in range(2):
            at = pl.multiple_of(window_ref[0, 2 * known + h] * slots, slots)
            rows = pl.ds(at, slots)
            pooled[rows, :] += got[h * slots : (h + 1) * slots]

    pairs_per_step = len(ids) * rows_per_chunk // 2
    stages = (stage_a, stage_b)
    window_copy.wait()

    def step(i, carry):
        for j in range(len(ids)):
            fetch(0, j).wait()
            for k in range(rows_per_chunk // 2):
                n = j * rows_per_chunk // 2 + k
                pool(i * pairs_per_step + n - 1, stages[(n + 1) % 2])
                gather(ids[j], 2 * k, stages[n % 2])
            fetch((i + 1) * len(ids) + j, j).start()
        return carry

    steps = (used + 2 * pairs_per_step - 1) // (2 * pairs_per_step)
    lax.fori_loop(0, steps, step, 0)
    pool(steps * pairs_per_step - 1, stage_b)
    for j in range(len(ids)):
        fetch(0, j).wait()

    weight_copy.wait()
    inverse_copy.wait()
    part = 256
    windows = part // WIN

    def finish(i, carry):
        at = pl.multiple_of(i * part, part)
        own = own_ref[pl.ds(at, part), :]

        def weight(r):
            return jnp.concatenate([weight_ref[r, 0], weight_ref[r, 1]], axis=1)

        total = bias_ref[...] + jnp.dot(
            own, weight(relations), preferred_element_type=jnp.float32
        )
        base = pl.multiple_of(i * windows * slots, windows * slots)
        sums = pooled[pl.ds(base, windows * slots), :].reshape(windows, relations, WIN, width)
        scale = inverse_ref[pl.ds(base, windows * slots), :].reshape(
            windows, relations, WIN, LANES
        )
        for r in range(relations):
            inverse = scale[:, r].reshape(part, LANES)
            sums_r = sums[:, r].reshape(part, width)
            mean = jnp.concatenate(
                [sums_r[:, :LANES] * inverse, sums_r[:, LANES:] * inverse], axis=1
            ).astype(jnp.bfloat16)
            total = total + jnp.dot(mean, weight(r), preferred_element_type=jnp.float32)
        if relu:
            total = jnp.maximum(total, 0.0)
        out_ref[pl.ds(at, part), :] = total.astype(jnp.bfloat16)
        return carry

    lax.fori_loop(0, nodes // part, finish, 0)


def relational_layer(
    layer, rows, received, count, sources, targets, relation_ids, weights, inverse, bias
):
    nodes, width = rows.shape
    relations = weights.shape[1] - 1
    table_rows = 2 * (nodes + received.shape[0])
    pieces = 4
    return pl.pallas_call(
        functools.partial(layer_body, layer == 0, layer),
        out_shape=jax.ShapeDtypeStruct((nodes, width), jnp.bfloat16),
        in_specs=[SMEM] + [ANY] * 8,
        out_specs=VMEM,
        scratch_shapes=[
            pltpu.VMEM((table_rows, LANES), jnp.float32),
            pltpu.VMEM((nodes * relations, width), jnp.float32),
            pltpu.VMEM((nodes * relations, LANES), jnp.float32),
            pltpu.VMEM((4 * LANES, LANES), jnp.float32),
            pltpu.VMEM((4 * LANES, LANES), jnp.float32),
            pltpu.VMEM(rows.shape, rows.dtype),
            pltpu.VMEM(received.shape, received.dtype),
            pltpu.VMEM(weights.shape[1:], weights.dtype),
            pltpu.VMEM(sources.shape, sources.dtype),
            pltpu.VMEM((8, LANES), sources.dtype),
            pltpu.SMEM((8, LANES), sources.dtype),
            pltpu.SMEM((CHUNK_BLOCKS, LANES), sources.dtype),
            pltpu.SMEM((CHUNK_BLOCKS, LANES), sources.dtype),
            pltpu.SemaphoreType.DMA,
            pltpu.SemaphoreType.DMA((pieces,)),
            pltpu.SemaphoreType.DMA,
            pltpu.SemaphoreType.DMA,
            pltpu.SemaphoreType.DMA,
            pltpu.SemaphoreType.DMA((2,)),
            pltpu.VMEM(sources.shape, sources.dtype),
            pltpu.VMEM(sources.shape, sources.dtype),
            pltpu.VMEM(sources.shape, sources.dtype),
            pltpu.VMEM((1, width), jnp.float32),
            pltpu.SemaphoreType.DMA((4,)),
        ],
        compiler_params=pltpu.CompilerParams(
            vmem_limit_bytes=LIMIT,
        ),
        name="relational_layer",
    )(
        count, sources, targets, relation_ids, rows, received, weights, inverse,
        bias.reshape(1, width),
    )


def shards(
    features,
    edge_source,
    edge_relation,
    edge_target,
    block_count,
    send_list,
    bases_first,
    self_first,
    coef_first,
    bias_first,
    bases_second,
    self_second,
    coef_second,
    bias_second,
):
    edges = (block_count, edge_source[0], edge_target[0], edge_relation[0])
    turned = jnp.swapaxes(send_list[0], 0, 1)
    width = features.shape[1]
    received, full, inverse = exchange(
        turned,
        features,
        (coef_first, bases_first, self_first, coef_second, bases_second, self_second),
        (block_count, edge_target[0], edge_relation[0]),
    )
    full = full.reshape(full.shape[:3] + (width, LANES))
    hidden = relational_layer(
        0, features, received.reshape(-1, width), *edges, full, inverse, bias_first
    )
    (received,) = exchange(turned, hidden)
    return relational_layer(
        1, hidden, received.reshape(-1, width), *edges, full, inverse, bias_second
    )


def solution(mesh):
    placed = (
        P("dom", None),
        P("dom", None, None),
        P("dom", None, None),
        P("dom", None, None),
        P("dom"),
        P("dom", None, None),
        P(None, "dom", None),
        P("dom", None),
        P(),
        P(),
        P(None, "dom", None),
        P("dom", None),
        P(),
        P(),
    )
    return jax.shard_map(
        shards, mesh=mesh, in_specs=placed, out_specs=P("dom", None), check_vma=False
    )
```

```python
import functools

import jax
import jax.numpy as jnp
from jax import lax
from jax.experimental import pallas as pl
from jax.experimental.pallas import tpu as pltpu
from jax.sharding import PartitionSpec as P

WIN = 16
LANES = 128
VMEM = pl.BlockSpec(memory_space=pltpu.VMEM)
SMEM = pl.BlockSpec(memory_space=pltpu.SMEM)
LIMIT = 60 * 1024 * 1024


def mix_weights(layer, coef_ref, bases_ref, self_ref, part_ref):
    relations = coef_ref.shape[0]
    rows = []
    for i in range(2):
        bases = bases_ref[:, i, :].astype(jnp.float32)
        rows.append(
            jnp.dot(
                coef_ref[...],
                bases,
                precision=lax.Precision.HIGHEST,
                preferred_element_type=jnp.float32,
            )
        )
    for h in range(2):
        lanes = slice(h * LANES, (h + 1) * LANES)
        for r in range(relations):
            both = jnp.concatenate([row[r : r + 1, lanes] for row in rows], axis=0)
            part_ref[layer, r, h] = both.astype(jnp.bfloat16)
        part_ref[layer, relations, h] = self_ref[:, lanes]


MESH = pl.DeviceIdType.MESH
ANY = pl.BlockSpec(memory_space=pl.ANY)
GROUP = 8
FIRST_GROUPS = 6
CHUNK_BLOCKS = 16


def rows_of_group(group, send_ref, rows_ref, out_ref):
    slots = send_ref.shape[1]
    nodes, width = rows_ref.shape
    ids = send_ref[pl.ds(pl.multiple_of(group * GROUP, GROUP), GROUP), :]
    hot = (
        (ids[:, :, None] == lax.broadcasted_iota(jnp.int32, (GROUP, slots, nodes), 2))
        .astype(jnp.float32)
        .astype(jnp.bfloat16)
        .reshape(GROUP * slots, nodes)
    )
    got = jnp.dot(hot, rows_ref[...], preferred_element_type=jnp.float32)
    out_ref[pl.ds(group * GROUP, GROUP)] = got.astype(jnp.bfloat16).reshape(GROUP, slots, width)


def remote(src, dst, send_sem, recv_sem, to):
    return pltpu.make_async_remote_copy(
        src_ref=src,
        dst_ref=dst,
        send_sem=send_sem,
        recv_sem=recv_sem,
        device_id=(to,),
        device_id_type=MESH,
    )


def tally_slots(target_ref, relation_ref, tally_ref):
    blocks, block_width = target_ref.shape
    slots = tally_ref.shape[1]
    lane = lax.broadcasted_iota(jnp.int32, (8, 2 * block_width), 1) // block_width
    row = lax.broadcasted_iota(jnp.int32, (8, 2 * block_width), 0)
    slot_ids = lax.broadcasted_iota(jnp.int32, (slots, 2 * block_width), 0)

    def tally(g, carry):
        at = pl.ds(pl.multiple_of(8 * g, 8), 8)
        slot = relation_ref[at, :] * WIN + lax.bitwise_and(target_ref[at, :], WIN - 1)
        total = jnp.zeros((8, slots), jnp.float32)
        for p in range(4):
            both = jnp.concatenate([slot[2 * p : 2 * p + 1], slot[2 * p + 1 : 2 * p + 2]], axis=1)
            hot = (both == slot_ids).astype(jnp.float32).astype(jnp.bfloat16)
            pick = (row == lane + 2 * p).astype(jnp.float32).astype(jnp.bfloat16)
            total = total + lax.dot_general(
                pick, hot, (((1,), (1,)), ((), ())), preferred_element_type=jnp.float32
            )
        tally_ref[at, :] = total
        return carry

    lax.fori_loop(0, blocks // 8, tally, 0)


def invert_degrees(count_ref, target_ref, tally_ref, windows):
    blocks = target_ref.shape[0]
    window = lax.shift_right_logical(target_ref[...].T[:1, :], 4)
    in_use = lax.broadcasted_iota(jnp.int32, (windows, blocks), 1) < count_ref[0]
    same = window == lax.broadcasted_iota(jnp.int32, (windows, blocks), 0)
    held = jnp.logical_and(same, in_use).astype(jnp.float32).astype(jnp.bfloat16)
    degree = jnp.dot(
        held, tally_ref[...].astype(jnp.bfloat16), preferred_element_type=jnp.float32
    )
    tally_ref[:windows, :] = 1.0 / jnp.maximum(degree, 1.0)


def spread_windows(first, last, tally_ref, inverse_ref):
    slots = tally_ref.shape[1]

    def spread(w, carry):
        row = jnp.broadcast_to(tally_ref[pl.ds(w, 1), :], (slots, slots))
        inverse_ref[pl.ds(pl.multiple_of(w * slots, slots), slots), :] = row.T
        return carry

    lax.fori_loop(first, last, spread, 0)


def exchange_body(count, with_weights, *refs):
    if with_weights:
        inputs, count_ref, refs = refs[:10], refs[10], refs[11:]
        (in_ref, full_ref, inverse_out, out_ref, send_ref, part_ref, tally_ref, inverse_ref,
         send_sem, recv_sem, plane_send, plane_recv, far_send, far_recv, core_send, core_recv,
         inverse_sem), refs = refs[:17], refs[17:]
        (turned_ref, rows_ref, coef_a, bases_a, self_a, coef_b, bases_b, self_b,
         target_ref, relation_ref) = refs[:10]
    else:
        inputs, refs = refs[:2], refs[2:]
        (in_ref, out_ref, send_ref, send_sem, recv_sem), refs = refs[:5], refs[5:]
        turned_ref, rows_ref = refs[:2]
    loads = [
        pltpu.make_async_copy(src, dst, refs[-1].at[i])
        for i, (src, dst) in enumerate(zip(inputs, refs[:-1]))
    ]
    me = lax.axis_index("dom")
    groups = count // GROUP
    barrier = pltpu.get_barrier_semaphore()

    for k in range(1, count):
        pl.semaphore_signal(
            barrier, inc=1, device_id=(lax.rem(me + k, count),), device_id_type=MESH
        )
    for load in loads:
        load.start()
    for load in loads:
        load.wait()

    def group_at(t):
        return lax.rem(me // GROUP + 5 * t, groups)

    def compute(t):
        rows_of_group(group_at(t), send_ref, rows_ref, out_ref)

    def send(t, first):
        for i in range(first, GROUP):
            to = group_at(t) * GROUP + lax.rem(me + i, GROUP)
            remote(out_ref.at[to], in_ref.at[me], send_sem, recv_sem, to).start()

    def step(t, carry):
        compute(t + 1)
        send(t, 0)
        return carry

    send_ref[...] = turned_ref[...].T
    if with_weights:
        mix_weights(0, coef_a, bases_a, self_a, part_ref)
        mix_weights(1, coef_b, bases_b, self_b, part_ref)
    compute(0)
    compute(1)
    pl.semaphore_wait(barrier, count - 1)
    if with_weights:
        core = lax.rem(me, 2)
        x = lax.rem(me // 2, 4)
        y = lax.rem(me // 8, 4)
        z = me // 32
        pair = lax.rem(me, 8)
        mine = pltpu.make_async_copy(
            part_ref.at[core], full_ref.at[core, :, :, z, y, pair], plane_recv
        )
        mine.start()

        def spread(layer):
            def one(k, carry):
                column = lax.rem(x + k, 4)
                if layer == 0:
                    line = (z * 4 + lax.rem(y + k // 4, 4)) * 4
                else:
                    line = (lax.rem(z + k // 4, 4) * 4 + y) * 4
                remote(
                    part_ref.at[layer],
                    full_ref.at[layer, :, :, z, y, pair],
                    plane_send.at[jnp.where(core == layer, 0, 1)],
                    plane_recv,
                    (line + column) * 2 + layer,
                ).start()
                return carry

            lax.fori_loop(jnp.where(core == layer, 1, 0), 16, one, 0)

        spread(0)
        spread(1)
    send(0, 1)
    if not with_weights:
        lax.fori_loop(1, groups - 1, step, 0)
    else:
        lax.fori_loop(1, FIRST_GROUPS, step, 0)
        arrived = full_ref.at[0, :, :, 0]
        pltpu.make_async_copy(arrived, arrived, plane_recv).wait()

        def slab_of(layer, back):
            if layer == 0:
                return full_ref.at[0, :, :, lax.rem(z + 4 - back, 4)]
            return full_ref.at[1, :, :, :, lax.rem(y + 4 - back, 4)]

        def far(layer, k):
            slab = slab_of(layer, 0)
            if layer == 0:
                to = lax.rem(me + 32 * k, count)
            else:
                to = z * 32 + lax.rem(y + k, 4) * 8 + pair
            return remote(slab, slab, far_send.at[k], far_recv.at[k], to)

        def across(layer, k):
            slab = slab_of(layer, k)
            return remote(slab, slab, core_send.at[k], core_recv.at[k], me + 1 - 2 * core)

        for layer in range(2):
            @pl.when(core == layer)
            def _():
                for k in (1, 3, 2):
                    far(layer, k).start()
                across(layer, 0).start()

        lax.fori_loop(FIRST_GROUPS, groups - 1, step, 0)
    send(groups - 1, 0)
    if with_weights:
        tally_slots(target_ref, relation_ref, tally_ref)
        slots = tally_ref.shape[1]
        windows = inverse_ref.shape[0] // slots
        quarter = windows // 4
        invert_degrees(count_ref, target_ref, tally_ref, windows)

        def put(q):
            rows = pl.ds(q * quarter * slots, quarter * slots)
            return pltpu.make_async_copy(
                inverse_ref.at[rows], inverse_out.at[rows], inverse_sem.at[q]
            )

        for q in range(4):
            spread_windows(q * quarter, (q + 1) * quarter, tally_ref, inverse_ref)
            if q > 0:
                put(q - 1).start()
        for layer in range(2):
            @pl.when(core == layer)
            def _():
                for k in (1, 3, 2):
                    far(layer, k).wait_recv()
                    across(layer, k).start()
        for layer in range(2):
            @pl.when(core == layer)
            def _():
                for k in (1, 3, 2):
                    far(layer, k).wait_send()
                for k in (0, 1, 3, 2):
                    across(layer, k).wait()
        put(3).start()
        for q in range(4):
            put(q).wait()
        gone = full_ref.at[0, :, :, 0:3, 0, 0:5]
        pltpu.make_async_copy(gone, gone, plane_send.at[0]).wait()
        gone = full_ref.at[0, :, :, 0:2, 0]
        pltpu.make_async_copy(gone, gone, plane_send.at[1]).wait()
    some = pl.ds(0, count - 1)
    pltpu.make_async_copy(in_ref.at[some], in_ref.at[some], recv_sem).wait()
    pltpu.make_async_copy(out_ref.at[some], out_ref.at[some], send_sem).wait()


def exchange(turned, rows, weights=(), edges=()):
    slots, count = turned.shape
    loaded = (turned, rows, *weights, *edges[1:])
    block = (count, slots, rows.shape[1])
    out_shape = [jax.ShapeDtypeStruct(block, rows.dtype)]
    scratch = [pltpu.VMEM(block, rows.dtype), pltpu.VMEM((count, slots), turned.dtype)]
    sems = [pltpu.SemaphoreType.DMA] * 2
    if weights:
        matrices = weights[0].shape[0] + 1
        halves = rows.shape[1] // LANES
        out_shape.append(
            jax.ShapeDtypeStruct((2, matrices, halves, 4, 4, 8, 2, LANES), rows.dtype)
        )
        slots = (matrices - 1) * WIN
        scratch.append(pltpu.VMEM((2, matrices, halves, 2, LANES), rows.dtype))
        scratch.append(pltpu.VMEM((edges[1].shape[0], slots), jnp.float32))
        inverse = (rows.shape[0] * (matrices - 1), LANES)
        scratch.append(pltpu.VMEM(inverse, jnp.float32))
        out_shape.append(jax.ShapeDtypeStruct(inverse, jnp.float32))
        sems += [pltpu.SemaphoreType.DMA((2,)), pltpu.SemaphoreType.DMA]
        sems += [pltpu.SemaphoreType.DMA((4,))] * 5
    return pl.pallas_call(
        functools.partial(exchange_body, count, bool(weights)),
        out_shape=out_shape,
        in_specs=[ANY] * len(loaded) + [SMEM] * len(edges[:1]),
        out_specs=[ANY] * len(out_shape),
        scratch_shapes=scratch
        + sems
        + [pltpu.VMEM(array.shape, array.dtype) for array in loaded]
        + [pltpu.SemaphoreType.DMA((len(loaded),))],
        compiler_params=pltpu.CompilerParams(
            collective_id=0 if weights else 1,
            has_side_effects=True,
            vmem_limit_bytes=LIMIT,
        ),
        name="exchange_weights" if weights else "exchange",
    )(*loaded, *edges[:1])


def layer_body(
    relu,
    layer,
    count_ref,
    source_hbm,
    target_hbm,
    relation_hbm,
    own_hbm,
    recv_hbm,
    weight_hbm,
    inverse_hbm,
    bias_hbm,
    out_hbm,
    table,
    pooled,
    inverse_ref,
    stage_a,
    stage_b,
    own_ref,
    recv_ref,
    weight_ref,
    doubled,
    window_row,
    window_ref,
    ids_0,
    ids_1,
    own_sem,
    recv_sem,
    weight_sem,
    inverse_sem,
    window_sem,
    ids_sem,
    source_ref,
    target_ref,
    relation_ref,
    bias_ref,
    small_sem,
    out_ref,
    out_sem,
):
    nodes, width = own_ref.shape
    relations = weight_ref.shape[0] - 1
    blocks, block_width = target_ref.shape
    slots = WIN * relations
    chunk = 256
    pieces = recv_sem.shape[0]
    piece = recv_ref.shape[0] // pieces

    small = [
        pltpu.make_async_copy(src, dst, small_sem.at[i])
        for i, (src, dst) in enumerate(
            [
                (source_hbm, source_ref),
                (target_hbm, target_ref),
                (relation_hbm, relation_ref),
                (bias_hbm, bias_ref),
            ]
        )
    ]
    for copy in small:
        copy.start()
    own_copy = pltpu.make_async_copy(own_hbm, own_ref, own_sem)
    own_copy.start()
    recv_copies = []
    for p in range(pieces):
        rows = pl.ds(p * piece, piece)
        copy = pltpu.make_async_copy(recv_hbm.at[rows], recv_ref.at[rows], recv_sem.at[p])
        copy.start()
        recv_copies.append(copy)
    weight_copy = pltpu.make_async_copy(weight_hbm.at[layer], weight_ref, weight_sem)
    inverse_copy = pltpu.make_async_copy(inverse_hbm, inverse_ref, inverse_sem)
    for copy in small:
        copy.wait()

    rows_per_chunk = ids_0.shape[0]
    chunks = blocks // rows_per_chunk
    doubled[...] = source_ref[...] * 2
    first = target_ref[...].T
    window_row[...] = lax.shift_right_logical(first[:8, :], 4)

    def clear(i, carry):
        at = pl.multiple_of(i * slots, slots)
        pooled[pl.ds(at, slots), :] = jnp.zeros((slots, width), jnp.float32)
        return carry

    lax.fori_loop(0, nodes // WIN, clear, 0)
    stage_b[...] = jnp.zeros_like(stage_b)

    ids = (ids_0, ids_1)

    def fetch(chunk, j):
        first_row = pl.multiple_of(
            jnp.minimum(chunk, chunks - 1) * rows_per_chunk, rows_per_chunk
        )
        return pltpu.make_async_copy(
            doubled.at[pl.ds(first_row, rows_per_chunk)], ids[j], ids_sem.at[j]
        )

    window_copy = pltpu.make_async_copy(window_row, window_ref, window_sem)
    window_copy.start()
    for j in range(len(ids)):
        fetch(j, j).start()

    def fill(src_ref, first, last, base):
        def step(i, carry):
            rows = src_ref[pl.ds(pl.multiple_of(i * chunk, chunk), chunk), :].astype(jnp.float32)
            at = pl.multiple_of(base + i * 2 * chunk, 2 * chunk)
            table[pl.ds(at, chunk, stride=2), :] = rows[:, :LANES]
            table[pl.ds(at + 1, chunk, stride=2), :] = rows[:, LANES:]
            return carry

        lax.fori_loop(first, last, step, 0)

    own_copy.wait()
    fill(own_ref, 0, nodes // chunk, 0)
    for p in range(pieces):
        recv_copies[p].wait()
        fill(recv_ref, p * piece // chunk, (p + 1) * piece // chunk, 2 * nodes)
    weight_copy.start()
    inverse_copy.start()

    used = count_ref[0]

    def gather(id_ref, first_row, stage):
        for h in range(2):
            for e in range(block_width):
                at = pl.multiple_of(id_ref[first_row + h, e], 2)
                stage[pl.ds(2 * (h * block_width + e), 2), :] = table[pl.ds(at, 2), :]

    def pool(pair, stage):
        known = jnp.maximum(pair, 0)
        slot = []
        for h in range(2):
            row = pl.ds(2 * known + h, 1)
            in_use = jnp.logical_and(pair >= 0, 2 * pair + h < used)
            shift = jnp.where(in_use, h * slots, 2 * slots)
            slot.append(
                relation_ref[row, :] * WIN + lax.bitwise_and(target_ref[row, :], WIN - 1) + shift
            )
        both = jnp.concatenate(slot, axis=1)
        hot = (
            both == lax.broadcasted_iota(jnp.int32, (2 * slots, 2 * block_width), 0)
        ).astype(jnp.float32).astype(jnp.bfloat16)
        edges = 2 * block_width
        data = jnp.concatenate(
            [
                stage[pl.ds(0, edges, stride=2), :].astype(jnp.bfloat16),
                stage[pl.ds(1, edges, stride=2), :].astype(jnp.bfloat16),
            ],
            axis=1,
        )
        got = jnp.dot(hot, data, preferred_element_type=jnp.float32)
        for h in range(2):
            at = pl.multiple_of(window_ref[0, 2 * known + h] * slots, slots)
            rows = pl.ds(at, slots)
            pooled[rows, :] += got[h * slots : (h + 1) * slots]

    pairs_per_step = len(ids) * rows_per_chunk // 2
    stages = (stage_a, stage_b)
    window_copy.wait()

    def step(i, carry):
        for j in range(len(ids)):
            fetch(0, j).wait()
            for k in range(rows_per_chunk // 2):
                n = j * rows_per_chunk // 2 + k
                pool(i * pairs_per_step + n - 1, stages[(n + 1) % 2])
                gather(ids[j], 2 * k, stages[n % 2])
            fetch((i + 1) * len(ids) + j, j).start()
        return carry

    steps = (used + 2 * pairs_per_step - 1) // (2 * pairs_per_step)
    lax.fori_loop(0, steps, step, 0)
    pool(steps * pairs_per_step - 1, stage_b)
    for j in range(len(ids)):
        fetch(0, j).wait()

    weight_copy.wait()
    inverse_copy.wait()
    part = 256
    windows = part // WIN

    def put(i):
        rows = pl.ds(pl.multiple_of(i * part, part), part)
        return pltpu.make_async_copy(out_ref.at[rows], out_hbm.at[rows], out_sem.at[i])

    def finish(i, carry):
        at = pl.multiple_of(i * part, part)
        own = own_ref[pl.ds(at, part), :]

        def weight(r):
            return jnp.concatenate([weight_ref[r, 0], weight_ref[r, 1]], axis=1)

        total = bias_ref[...] + jnp.dot(
            own, weight(relations), preferred_element_type=jnp.float32
        )
        base = pl.multiple_of(i * windows * slots, windows * slots)
        sums = pooled[pl.ds(base, windows * slots), :].reshape(windows, relations, WIN, width)
        scale = inverse_ref[pl.ds(base, windows * slots), :].reshape(
            windows, relations, WIN, LANES
        )
        for r in range(relations):
            inverse = scale[:, r].reshape(part, LANES)
            sums_r = sums[:, r].reshape(part, width)
            mean = jnp.concatenate(
                [sums_r[:, :LANES] * inverse, sums_r[:, LANES:] * inverse], axis=1
            ).astype(jnp.bfloat16)
            total = total + jnp.dot(mean, weight(r), preferred_element_type=jnp.float32)
        if relu:
            total = jnp.maximum(total, 0.0)
        out_ref[pl.ds(at, part), :] = total.astype(jnp.bfloat16)

        @pl.when(i > 0)
        def _():
            put(i - 1).start()

        return carry

    parts = nodes // part
    lax.fori_loop(0, parts, finish, 0)
    put(parts - 1).start()
    for i in range(parts):
        put(i).wait()


def relational_layer(
    layer, rows, received, count, sources, targets, relation_ids, weights, inverse, bias
):
    nodes, width = rows.shape
    relations = weights.shape[1] - 1
    table_rows = 2 * (nodes + received.shape[0])
    pieces = 4
    return pl.pallas_call(
        functools.partial(layer_body, layer == 0, layer),
        out_shape=jax.ShapeDtypeStruct((nodes, width), jnp.bfloat16),
        in_specs=[SMEM] + [ANY] * 8,
        out_specs=ANY,
        scratch_shapes=[
            pltpu.VMEM((table_rows, LANES), jnp.float32),
            pltpu.VMEM((nodes * relations, width), jnp.float32),
            pltpu.VMEM((nodes * relations, LANES), jnp.float32),
            pltpu.VMEM((4 * LANES, LANES), jnp.float32),
            pltpu.VMEM((4 * LANES, LANES), jnp.float32),
            pltpu.VMEM(rows.shape, rows.dtype),
            pltpu.VMEM(received.shape, received.dtype),
            pltpu.VMEM(weights.shape[1:], weights.dtype),
            pltpu.VMEM(sources.shape, sources.dtype),
            pltpu.VMEM((8, LANES), sources.dtype),
            pltpu.SMEM((8, LANES), sources.dtype),
            pltpu.SMEM((CHUNK_BLOCKS, LANES), sources.dtype),
            pltpu.SMEM((CHUNK_BLOCKS, LANES), sources.dtype),
            pltpu.SemaphoreType.DMA,
            pltpu.SemaphoreType.DMA((pieces,)),
            pltpu.SemaphoreType.DMA,
            pltpu.SemaphoreType.DMA,
            pltpu.SemaphoreType.DMA,
            pltpu.SemaphoreType.DMA((2,)),
            pltpu.VMEM(sources.shape, sources.dtype),
            pltpu.VMEM(sources.shape, sources.dtype),
            pltpu.VMEM(sources.shape, sources.dtype),
            pltpu.VMEM((1, width), jnp.float32),
            pltpu.SemaphoreType.DMA((4,)),
            pltpu.VMEM((nodes, width), jnp.bfloat16),
            pltpu.SemaphoreType.DMA((4,)),
        ],
        compiler_params=pltpu.CompilerParams(
            vmem_limit_bytes=LIMIT,
        ),
        name="relational_layer",
    )(
        count, sources, targets, relation_ids, rows, received, weights, inverse,
        bias.reshape(1, width),
    )


def shards(
    features,
    edge_source,
    edge_relation,
    edge_target,
    block_count,
    send_list,
    bases_first,
    self_first,
    coef_first,
    bias_first,
    bases_second,
    self_second,
    coef_second,
    bias_second,
):
    edges = (block_count, edge_source[0], edge_target[0], edge_relation[0])
    turned = jnp.swapaxes(send_list[0], 0, 1)
    width = features.shape[1]
    received, full, inverse = exchange(
        turned,
        features,
        (coef_first, bases_first, self_first, coef_second, bases_second, self_second),
        (block_count, edge_target[0], edge_relation[0]),
    )
    full = full.reshape(full.shape[:3] + (width, LANES))
    hidden = relational_layer(
        0, features, received.reshape(-1, width), *edges, full, inverse, bias_first
    )
    (received,) = exchange(turned, hidden)
    return relational_layer(
        1, hidden, received.reshape(-1, width), *edges, full, inverse, bias_second
    )


def solution(mesh):
    placed = (
        P("dom", None),
        P("dom", None, None),
        P("dom", None, None),
        P("dom", None, None),
        P("dom"),
        P("dom", None, None),
        P(None, "dom", None),
        P("dom", None),
        P(),
        P(),
        P(None, "dom", None),
        P("dom", None),
        P(),
        P(),
    )
    return jax.shard_map(
        shards, mesh=mesh, in_specs=placed, out_specs=P("dom", None), check_vma=False
    )
```
